256 devices in a mesh: chain: 16 (over z, core), dp: 16 (over y, x).
Axes of the slice: x: 4, y: 4, z: 8, core: 2. Of those that a mesh axis runs over, the one named last changes fastest.
Arguments:
- images_in: float32 [16, 1024, 1024], P('chain', 'dp'), may hold values from -8 to 8
- images_mid: float32 [16, 1024, 1024], P('chain', 'dp'), may hold values from -8 to 8
- images_out: float32 [16, 1024, 1000], P('chain', 'dp'), may hold values from -8 to 8
- ends_in: float32 [2, 1024, 1024], P(None, 'dp'), may hold values from -8 to 8
- ends_mid: float32 [2, 1024, 1024], P(None, 'dp'), may hold values from -8 to 8
- ends_out: float32 [2, 1024, 1000], P(None, 'dp'), may hold values from -8 to 8
- data_pool: bfloat16 [28672, 1024], P('dp'), may hold values from -6 to 6
- batch_rows: int32 [16, 14336], P('chain', 'dp'), may hold values from 0 to 1791
- labels: int32 [16, 14336], P('chain', 'dp'), may hold values from 0 to 999
- climbing: int32 [16], P('chain'), may hold values 0 or 1
Outputs:
- new_in: float32 [16, 1024, 1024], P('chain', 'dp')
- new_mid: float32 [16, 1024, 1024], P('chain', 'dp')
- new_out: float32 [16, 1024, 1000], P('chain', 'dp')
- energies: float32 [16], P('chain')
- arc_share: float32 [16], P('chain')
- bend: float32 [16], P('chain')
The draws below stay inside these ranges and needn't reach their ends.
Inputs may be any that keep to these rules, and one draw needn't show every extreme that they name: batch_rows[i, b] names a row of the pool shard held by dp index b // 896.
All inputs are finite; a program needn't handle non-finite values. No bound on the sum of `climbing` on one device may be relied on, other than what follows from the above.
Results may differ from the reference program's by a relative error of at most 0.0023.
Values may be sent and summed in bfloat16 or wider, within the bound.
A program may use at most 128 MiB of HBM per device.

```python
import jax
import jax.numpy as jnp
from jax import lax

D = 1024
FF = 1024
C = 1000
B_DEV = 896
POOL = 1792
IMAGES = 16
BATCH = 14336
ROWS = 28672


def row_scale(count):
    top = 2.5
    return jnp.exp(jnp.log(top) * jnp.arange(count, dtype=jnp.float32) / (count - 1))


def band_ends(key, tag, shape):
    scale = row_scale(shape[0])[:, None]
    first = jax.random.normal(jax.random.fold_in(key, tag), shape, jnp.float32) * scale
    second = jax.random.normal(jax.random.fold_in(key, tag + 100), shape, jnp.float32) * scale
    return (jnp.clip(first, -7.5, 7.5), jnp.clip(second, -7.5, 7.5))


def band_images(key, tag, shape):
    first, second = band_ends(key, tag, shape)
    scale = row_scale(shape[0])[None, :, None]
    spacing = 1.0 + 2.0 * jnp.arange(IMAGES + 1, dtype=jnp.float32) / IMAGES
    along = jnp.cumsum(spacing)[:IMAGES] / jnp.sum(spacing)
    noise_key = jax.random.fold_in(key, tag + 200)
    noise = 0.03 * jax.random.normal(noise_key, (IMAGES,) + shape, jnp.float32)
    return first[None] + along[:, None, None] * (second - first)[None] + noise * scale


def draw_images_in(key, part):
    return band_images(key, 1, (D, FF))


def draw_images_mid(key, part):
    return band_images(key, 2, (FF, D))


def draw_images_out(key, part):
    return band_images(key, 3, (D, C))


def draw_ends_in(key, part):
    return jnp.stack(band_ends(key, 1, (D, FF)))


def draw_ends_mid(key, part):
    return jnp.stack(band_ends(key, 2, (FF, D)))


def draw_ends_out(key, part):
    return jnp.stack(band_ends(key, 3, (D, C)))


def plant(result, rng, least, high):
    dims = result.shape
    index_at = [jax.random.randint(jax.random.fold_in(rng, axis), (), 0, dims[axis]) for axis in range(len(dims))]
    result = result.at[tuple(index_at)].set(least)
    longest = dims.index(max(dims))
    index_at[longest] = (index_at[longest] + 1) % dims[longest]
    return result.at[tuple(index_at)].set(high)


def steps_of(rng, dims, shards, low, high):
    def one(axis_at, blocks):
        draws = jax.random.uniform(jax.random.fold_in(jax.random.fold_in(rng, 6), axis_at), (blocks,), jnp.float32, low / len(shards), high / len(shards))
        return jnp.repeat(jnp.exp(draws), dims[axis_at] // blocks).reshape((-1,) + (1,) * (len(dims) - axis_at - 1))

    gain = one(*shards[0])
    for cut in shards[1:]:
        gain = gain * one(*cut)
    return gain


def centred(key, dims, width, bound, split=(), kind=jnp.bfloat16):
    factor_of = steps_of(key, dims, split, -0.22, 0.18) if split else 1.0
    values = jax.random.normal(key, dims, jnp.float32) * width * factor_of
    return jnp.minimum(jnp.maximum(values, -bound), bound).astype(kind)


def setup_inputs(seed: int = 0) -> dict:
    seeds = jax.random.split(jax.random.key(seed), 11)
    return {
        "images_in": draw_images_in(jax.random.fold_in(seeds[10], 71), 0),
        "images_mid": draw_images_mid(jax.random.fold_in(seeds[10], 71), 0),
        "images_out": draw_images_out(jax.random.fold_in(seeds[10], 71), 0),
        "ends_in": draw_ends_in(jax.random.fold_in(seeds[10], 71), 0),
        "ends_mid": draw_ends_mid(jax.random.fold_in(seeds[10], 71), 0),
        "ends_out": draw_ends_out(jax.random.fold_in(seeds[10], 71), 0),
        "data_pool": centred(seeds[6], (ROWS, D), 1.0, 6.0, ((0, 16),)),
        "batch_rows": plant(jax.random.randint(seeds[7], (IMAGES, BATCH), 0, POOL), jax.random.fold_in(seeds[7], 1), 0, POOL - 1).astype(jnp.int32),
        "labels": plant(jax.random.randint(seeds[8], (IMAGES, BATCH), 0, C), jax.random.fold_in(seeds[8], 1), 0, C - 1).astype(jnp.int32),
        "climbing": plant((jax.random.randint(seeds[9], (IMAGES,), 0, 4) < 1).astype(jnp.int32), jax.random.fold_in(seeds[9], 1), 0, 1),
    }


SPRING = 0.03
EPS = 1e-06

def silu_slope(pre):
    sig = jax.nn.sigmoid(pre)
    return sig * (1.0 + pre * (1.0 - sig))

def image_terms(packed, data_pool):
    p_in, p_mid, p_out, picks, labs = packed
    w_in = (p_in * D ** (-0.5)).astype(jnp.bfloat16)
    w_mid = (p_mid * FF ** (-0.5)).astype(jnp.bfloat16)
    w_out = (p_out * D ** (-0.5)).astype(jnp.bfloat16)
    owner = (jnp.arange(BATCH, dtype=jnp.int32) // B_DEV).astype(jnp.int32)
    rows = data_pool[owner * POOL + picks]
    pre = jnp.dot(rows, w_in, preferred_element_type=jnp.float32)
    hid = jax.nn.silu(pre).astype(jnp.bfloat16)
    resid = (rows.astype(jnp.float32) + jnp.dot(hid, w_mid, preferred_element_type=jnp.float32)).astype(jnp.bfloat16)
    logits = jnp.dot(resid, w_out, preferred_element_type=jnp.float32)
    target = (labs[:, None] == jnp.arange(C, dtype=jnp.int32)[None, :]).astype(jnp.float32)
    err = logits - target
    norm = 1.0 / (BATCH * C)
    energy = 0.5 * norm * jnp.sum(err * err)
    d_logits = (err * norm).astype(jnp.bfloat16)
    d_resid = jnp.dot(d_logits, w_out.T, preferred_element_type=jnp.float32).astype(jnp.bfloat16)
    d_pre = (jnp.dot(d_resid, w_mid.T, preferred_element_type=jnp.float32) * silu_slope(pre)).astype(jnp.bfloat16)
    g_in = jnp.dot(rows.T, d_pre, preferred_element_type=jnp.float32) * D ** (-0.5)
    g_mid = jnp.dot(hid.T, d_resid, preferred_element_type=jnp.float32) * FF ** (-0.5)
    g_out = jnp.dot(resid.T, d_logits, preferred_element_type=jnp.float32) * D ** (-0.5)
    return (g_in, g_mid, g_out, energy)

def inner(first, second):
    total = jnp.zeros((first[0].shape[0],), jnp.float32)
    for left, right in zip(first, second):
        total = total + lax.optimization_barrier(jnp.sum(left * right, axis=(1, 2)))
    return total

def reference(images_in, images_mid, images_out, ends_in, ends_mid, ends_out, data_pool, batch_rows, labels, climbing):
    g_in, g_mid, g_out, energies = lax.map(lambda packed: image_terms(packed, data_pool), (images_in, images_mid, images_out, batch_rows, labels))
    own = (images_in, images_mid, images_out)
    ends = (ends_in, ends_mid, ends_out)
    grads = (g_in, g_mid, g_out)
    before = tuple((jnp.concatenate([e[0:1], o[:-1]], axis=0) for e, o in zip(ends, own)))
    after = tuple((jnp.concatenate([o[1:], e[1:2]], axis=0) for e, o in zip(ends, own)))
    ahead = tuple((a - o for a, o in zip(after, own)))
    behind = tuple((o - b for o, b in zip(own, before)))
    len_ahead = jnp.sqrt(inner(ahead, ahead) + EPS)
    len_behind = jnp.sqrt(inner(behind, behind) + EPS)
    raw = tuple((a / len_ahead[:, None, None] + b / len_behind[:, None, None] for a, b in zip(ahead, behind)))
    raw_norm = jnp.sqrt(inner(raw, raw) + EPS)
    tau = tuple((r / raw_norm[:, None, None] for r in raw))
    along = inner(grads, tau)
    arc = jnp.cumsum(len_behind)
    band = jnp.sum(len_behind) + len_ahead[-1]
    order = jnp.arange(IMAGES, dtype=jnp.int32)
    target = (order + 1).astype(jnp.float32) / (IMAGES + 1) * band
    coef = jnp.where(climbing == 1, 2.0 * along, along + SPRING * (target - arc) / band)
    force = tuple((-g + coef[:, None, None] * t for g, t in zip(grads, tau)))
    force_len = jnp.sqrt(inner(force, force) + EPS)
    scale = band / (IMAGES + 1) / force_len
    new = tuple((o + scale[:, None, None] * f for o, f in zip(own, force)))
    return (new[0], new[1], new[2], energies, arc / band, 0.5 * raw_norm)
```

```python
import functools

import jax
import jax.numpy as jnp
from jax import lax
from jax.experimental import pallas as pl
from jax.experimental.pallas import tpu as pltpu
from jax.sharding import Mesh
from jax.sharding import PartitionSpec as P

DP = ("dp_0", "dp_1")
SPRING = 0.03
EPS = 1e-06
F32 = jnp.float32
BF16 = jnp.bfloat16
SIDE = 4
N_COPIES = 260


def mm(a, b):
    return jnp.dot(a, b, preferred_element_type=F32)


def mm_nt(a, b):
    return lax.dot_general(a, b, (((1,), (1,)), ((), ())), preferred_element_type=F32)


def mm_tn(a, b):
    return lax.dot_general(a, b, (((0,), (0,)), ((), ())), preferred_element_type=F32)


class Copies:
    def __init__(self, send, recv):
        self.send, self.recv, self.all = send, recv, []

    def start(self, src, dst, device):
        i = len(self.all)
        copy = pltpu.make_async_remote_copy(
            src_ref=src,
            dst_ref=dst,
            send_sem=self.send.at[i],
            recv_sem=self.recv.at[i],
            device_id=device,
            device_id_type=pl.DeviceIdType.MESH,
        )
        copy.start()
        self.all.append(copy)
        return copy


def kernel(
    dims,
    im_in, im_mid, im_out, en_in, en_mid, en_out, pool_hbm, rows_ref, labs_ref, climb_ref,
    up_in, up_mid, up_out, tab_ref,
    W, G, RA1, RAd, RAs, R1, RB1, RBd, RBs, gsh,
    own_in, own_mid, own_out, nb_in, nb_mid, nb_out, e_in, e_mid, e_out, AH, BH,
    pool, onehot, rcol, lcol, x, hid, slope, resid, dlog, dres, dpre,
    mine, sums, chain_mine, chain_tab,
    local_sem, send_sem, recv_sem,
):
    chain_n, batch, classes = dims
    rows = x.shape[0]
    width = x.shape[1]
    half_rows = rows // 2
    ci = lax.axis_index("chain")
    yi = lax.axis_index("dp_0")
    xi = lax.axis_index("dp_1")
    cp = Copies(send_sem, recv_sem)

    def at_x(step):
        return {"dp_1": lax.rem(xi + step, SIDE)}

    def at_y(step):
        return {"dp_0": lax.rem(yi + step, SIDE)}

    def xs(step):
        return lax.rem(xi + step, SIDE)

    def ys(step):
        return lax.rem(yi + step, SIDE)

    def at_chain(step):
        return {"chain": lax.rem(ci + step, chain_n)}

    loads = []

    def load(src, dst):
        c = pltpu.make_async_copy(src, dst, local_sem.at[len(loads)])
        c.start()
        loads.append(c)

    load(im_in.at[0], own_in)
    load(im_mid.at[0], own_mid)
    load(im_out.at[0], own_out)
    load(pool_hbm, pool)
    load(en_in, e_in)
    load(en_mid, e_mid)
    load(en_out, e_out)

    barrier = pltpu.get_barrier_semaphore()
    partners = [at_x(s) for s in (1, 2, 3)] + [at_y(s) for s in (1, 2, 3)]
    partners += [at_chain(s) for s in range(1, chain_n)]
    for device in partners:
        pl.semaphore_signal(barrier, inc=1, device_id=device, device_id_type=pl.DeviceIdType.MESH)

    factors = (width ** (-0.5), hid.shape[1] ** (-0.5), width ** (-0.5))
    edge = classes // 128 * 128
    for m, ref in enumerate((own_in, own_mid, own_out)):
        loads[m].wait()
        if m == 2:
            W[m, yi, xi, :, :, edge:] = jnp.zeros((2, 32, width - edge), BF16)
        n = ref.shape[1]
        W[m, yi, xi, :, :, :n] = (ref[...] * factors[m]).astype(BF16).reshape(2, 32, n)
    pl.semaphore_wait(barrier, len(partners))

    DIRS = (1, 3)

    def near(h, d):
        return at_x(d) if h == 0 else at_y(d)

    def far(h, d):
        return at_y(d) if h == 0 else at_x(d)

    def w_near(m, h, step):
        return W.at[m, yi, xs(step), h] if h == 0 else W.at[m, ys(step), xi, h]

    def w_near_half(m, h, step, k):
        r = pl.ds(16 * k, 16)
        return W.at[m, yi, xs(step), h, r] if h == 0 else W.at[m, ys(step), xi, h, r]

    def blocks(ref, m, h, step, k, cols=None):
        two = pl.ds(2 * k, 2)
        cols = pl.ds(0, ref.shape[-1]) if cols is None else cols
        if h == 0:
            return ref.at[m, ys(step), two, 0, :, cols]
        return ref.at[m, two, xs(step), 1, :, cols]

    BOTH = [(h, k) for h in (0, 1) for k in (0, 1)]
    p1, p1f, p2a, p2b, p2f = {}, {}, {}, {}, {}
    for m in range(3):
        for h, k in BOTH:
            src = w_near(m, h, 0)
            p1[m, h, k] = cp.start(src, src, near(h, DIRS[k]))

    nb = []
    for own, buf in ((own_in, nb_in), (own_mid, nb_mid), (own_out, nb_out)):
        nb.append(cp.start(own, buf.at[0], at_chain(1)))
        nb.append(cp.start(own, buf.at[1], at_chain(chain_n - 1)))

    def ag_near_forward(m):
        for h, k in BOTH:
            p1[m, h, k].wait_recv()
            src = w_near_half(m, h, SIDE - DIRS[k], k)
            p1f[m, h, k] = cp.start(src, src, near(h, DIRS[k]))

    def ag_far_start(m):
        for h, k in BOTH:
            p1f[m, h, k].wait_recv()
        for h, k in BOTH:
            src = blocks(W, m, h, 0, k)
            p2a[m, h, k] = cp.start(src, src, far(h, DIRS[k]))
        for h, k in BOTH:
            src = blocks(W, m, h, 0, 1 - k)
            p2b[m, h, k] = cp.start(src, src, far(h, DIRS[k]))

    def ag_far_forward(m):
        for h, k in BOTH:
            p2a[m, h, k].wait_recv()
            src = blocks(W, m, h, SIDE - DIRS[k], k)
            p2f[m, h, k] = cp.start(src, src, far(h, DIRS[k]))

    def ag_end(m):
        for h, k in BOTH:
            p2b[m, h, k].wait_recv()
            p2f[m, h, k].wait_recv()

    def weight(m):
        return W[m].reshape(width, width)

    def part(i):
        return pl.ds(i * half_rows, half_rows)

    for ref, col in ((rows_ref, rcol), (labs_ref, lcol)):
        for k in range(rows // 128):
            r = pl.ds(k * 128, 128)
            col[r, :] = jnp.transpose(jnp.broadcast_to(ref[:, r].astype(F32), (128, 128)))

    def lanes(c):
        return (lax.broadcasted_iota(jnp.int32, (1, 128), 1) + 128 * c).astype(F32)

    def pick_rows(i):
        for c in range(pool.shape[0] // 128):
            hit = rcol[part(i), :] == lanes(c)
            onehot[part(i), c * 128 : (c + 1) * 128] = jnp.where(hit, 1.0, 0.0).astype(BF16)
        x[part(i), :] = mm(onehot[part(i), :], pool[...]).astype(BF16)

    loads[3].wait()
    pick_rows(0)
    ag_near_forward(0)
    pick_rows(1)
    ag_near_forward(1)
    ag_near_forward(2)
    ag_far_start(0)

    for c in loads[4:]:
        c.wait()
    for c in nb:
        c.wait_recv()
    first, last = ci == 0, ci == chain_n - 1
    own = (own_in, own_mid, own_out)
    sq_a = sq_b = cross = jnp.zeros((1, 128), F32)

    def fold(v):
        v = jnp.sum(v, axis=0, keepdims=True)
        out = v[:, :128]
        for c in range(1, v.shape[1] // 128):
            out = out + v[:, c * 128 : (c + 1) * 128]
        return out

    for m, (e, b) in enumerate(((e_in, nb_in), (e_mid, nb_mid), (e_out, nb_out))):
        n = own[m].shape[1]
        o = own[m][...]
        if m == 2:
            AH[m, :, edge:] = jnp.zeros((o.shape[0], width - edge), F32)
            BH[m, :, edge:] = jnp.zeros((o.shape[0], width - edge), F32)
        AH[m, :, :n] = jnp.where(last, e[1], b[1]) - o
        BH[m, :, :n] = o - jnp.where(first, e[0], b[0])
        a, z = AH[m], BH[m]
        sq_a, sq_b, cross = sq_a + fold(a * a), sq_b + fold(z * z), cross + fold(a * z)

    def pack(*values):
        zero = jnp.zeros((8 - len(values), 128), F32)
        return jnp.concatenate([*values, zero], axis=0)

    def exchange(slot, tile, index, peers):
        mine[slot] = tile
        return [cp.start(mine.at[slot], sums.at[slot, index], device) for device in peers]

    def collect(slot, copies, index):
        for c in copies:
            c.wait_recv()
        sums[slot, index] = mine[slot]
        out = sums[slot, 0]
        for k in range(1, SIDE):
            out = out + sums[slot, k]
        return out

    x_peers = [at_x(s) for s in (1, 2, 3)]
    y_peers = [at_y(s) for s in (1, 2, 3)]
    early_x = exchange(0, pack(sq_b, sq_a, cross), xi, x_peers)
    ag_far_forward(0)
    ag_far_start(1)
    early_y = exchange(1, collect(0, early_x, xi), yi, y_peers)
    early = jnp.sum(collect(1, early_y, yi), axis=1, keepdims=True)
    sq_behind = jnp.broadcast_to(early[0:1], (1, 128))
    sq_ahead = jnp.broadcast_to(early[1:2], (1, 128))
    cross = jnp.broadcast_to(early[2:3], (1, 128))
    len_ahead = jnp.sqrt(sq_ahead + EPS)
    len_behind = jnp.sqrt(sq_behind + EPS)
    raw_sq = (
        sq_ahead / (len_ahead * len_ahead)
        + sq_behind / (len_behind * len_behind)
        + 2.0 * cross / (len_ahead * len_behind)
    )
    raw_len = jnp.sqrt(raw_sq + EPS)
    tau_sq = raw_sq / (raw_sq + EPS)
    chain_mine[...] = pack(len_behind, len_ahead)
    lengths = [
        cp.start(chain_mine, chain_tab.at[ci], at_chain(s)) for s in range(1, chain_n)
    ]

    def forward_in(i):
        pre = mm(x[part(i), :], weight(0))
        sig = jax.nn.sigmoid(pre)
        hid[part(i), :] = (pre * sig).astype(BF16)
        slope[part(i), :] = sig * (1.0 + pre * (1.0 - sig))

    def forward_mid(i):
        r = x[part(i), :].astype(F32) + mm(hid[part(i), :], weight(1))
        resid[part(i), :] = r.astype(BF16)

    norm = 1.0 / (batch * classes)

    def forward_out(i, energy):
        logits = mm(resid[part(i), :], weight(2))
        for c in range(width // 128):
            hit = lcol[part(i), :] == lanes(c)
            err = logits[:, c * 128 : (c + 1) * 128] - jnp.where(hit, 1.0, 0.0)
            energy = energy + jnp.sum(err * err, axis=0, keepdims=True)
            dlog[part(i), c * 128 : (c + 1) * 128] = (err * norm).astype(BF16)
        return energy

    ag_end(0)
    forward_in(0)
    ag_far_forward(1)
    ag_far_start(2)
    forward_in(1)
    for c in lengths:
        c.wait_recv()
    chain_tab[ci] = chain_mine[...]
    arc = jnp.zeros((1, 128), F32)
    band = jnp.zeros((1, 128), F32)
    for j in range(chain_n):
        piece = chain_tab[j, 0:1]
        arc = arc + jnp.where(j <= ci, piece, 0.0)
        band = band + piece
    band = band + chain_tab[chain_n - 1, 1:2]
    ag_end(1)
    forward_mid(0)
    forward_mid(1)
    ag_far_forward(2)
    ag_end(2)
    energy = forward_out(0, jnp.zeros((1, 128), F32))
    energy = forward_out(1, energy)

    COLS = width // 2
    PIECES = [(m, c) for m in (2, 1, 0) for c in (0, 1)]

    def cols_of(c):
        return pl.ds(c * COLS, COLS)

    def grad(p, left, right):
        m, c = PIECES[p]
        g = mm_tn(left[...], right[:, cols_of(c)]).astype(BF16)
        G[m, :, :, :, :, cols_of(c)] = g.reshape(SIDE, SIDE, 2, 32, COLS)

    a1, ad, a_s, b1, bd, bs = {}, {}, {}, {}, {}, {}

    def rs_start(p):
        m, c = PIECES[p]
        q = cols_of(c)
        for h, k in BOTH:
            dst = RA1.at[m, h, k, :, :, q]
            a1[p, h, k] = cp.start(blocks(G, m, h, 2, k, q), dst, far(h, DIRS[k]))
        for h, k in BOTH:
            dst = RAd.at[m, h, k, :, :, q]
            src = blocks(G, m, h, DIRS[k], 1 - k, q)
            ad[p, h, k] = cp.start(src, dst, far(h, DIRS[k]))

    def rs_far_sum(p):
        m, c = PIECES[p]
        q = cols_of(c)
        for h, k in BOTH:
            a1[p, h, k].wait_recv()
            mid = RA1.at[m, h, k, :, :, q]
            own_g = blocks(G, m, h, DIRS[k], k, q)
            mid[...] = (mid[...].astype(F32) + own_g[...].astype(F32)).astype(BF16)
            a_s[p, h, k] = cp.start(mid, RAs.at[m, h, k, :, :, q], far(h, DIRS[k]))

    def rs_near_start(p):
        m, c = PIECES[p]
        q = cols_of(c)
        for h in (0, 1):
            for k in (0, 1):
                ad[p, h, k].wait_recv()
                a_s[p, h, k].wait_recv()
            for k in (0, 1):
                total = blocks(G, m, h, 0, k, q)[...].astype(F32)
                total = total + RAs[m, h, k, :, :, q].astype(F32)
                total = total + RAd[m, h, 1 - k, :, :, q].astype(F32)
                R1[m, h, pl.ds(2 * k, 2), :, q] = total.astype(BF16)
            for k in (0, 1):
                step = ys if h else xs
                src = R1.at[m, h, step(2), pl.ds(16 * k, 16), q]
                b1[p, h, k] = cp.start(src, RB1.at[m, h, k, :, q], near(h, DIRS[k]))
            for k in (0, 1):
                src = R1.at[m, h, step(DIRS[k]), pl.ds(16 * (1 - k), 16), q]
                bd[p, h, k] = cp.start(src, RBd.at[m, h, k, :, q], near(h, DIRS[k]))

    def rs_near_sum(p):
        m, c = PIECES[p]
        q = cols_of(c)
        for h, k in BOTH:
            step = ys if h else xs
            b1[p, h, k].wait_recv()
            mid = RB1.at[m, h, k, :, q]
            own_r = R1[m, h, step(DIRS[k]), pl.ds(16 * k, 16), q]
            mid[...] = (mid[...].astype(F32) + own_r.astype(F32)).astype(BF16)
            bs[p, h, k] = cp.start(mid, RBs.at[m, h, k, :, q], near(h, DIRS[k]))

    dots = [jnp.zeros((1, 128), F32)] * 3

    def rs_end(p):
        m, c = PIECES[p]
        q = cols_of(c)
        for h in (0, 1):
            step = ys if h else xs
            for k in (0, 1):
                bd[p, h, k].wait_recv()
                bs[p, h, k].wait_recv()
            for k in (0, 1):
                total = R1[m, h, step(0), pl.ds(16 * k, 16), q].astype(F32)
                total = total + RBs[m, h, k, :, q].astype(F32)
                total = total + RBd[m, h, 1 - k, :, q].astype(F32)
                g = total * factors[m]
                r = pl.ds(32 * h + 16 * k, 16)
                gsh[m, r, q] = g
                dots[0] = dots[0] + fold(g * AH[m, r, q])
                dots[1] = dots[1] + fold(g * BH[m, r, q])
                dots[2] = dots[2] + fold(g * g)

    def back_resid(i):
        dres[part(i), :] = mm_nt(dlog[part(i), :], weight(2)).astype(BF16)

    def back_pre(i):
        d = mm_nt(dres[part(i), :], weight(1)) * slope[part(i), :]
        dpre[part(i), :] = d.astype(BF16)

    grad(0, resid, dlog)
    rs_start(0)
    grad(1, resid, dlog)
    rs_start(1)
    back_resid(0)
    rs_far_sum(0)
    back_resid(1)
    rs_far_sum(1)
    grad(2, hid, dres)
    rs_start(2)
    grad(3, hid, dres)
    rs_start(3)
    back_pre(0)
    rs_far_sum(2)
    back_pre(1)
    grad(4, x, dpre)
    rs_start(4)
    rs_far_sum(3)
    grad(5, x, dpre)
    rs_start(5)
    rs_near_start(0)
    rs_far_sum(4)
    rs_near_start(1)
    rs_far_sum(5)
    rs_near_start(2)
    rs_near_sum(0)
    rs_near_start(3)
    rs_near_sum(1)
    rs_near_start(4)
    rs_near_sum(2)
    rs_near_start(5)
    rs_near_sum(3)
    rs_end(0)
    rs_end(1)
    rs_near_sum(4)
    rs_end(2)
    rs_near_sum(5)
    rs_end(3)
    rs_end(4)
    rs_end(5)

    late_x = exchange(2, pack(*dots, energy), xi, x_peers)
    late_y = exchange(3, collect(2, late_x, xi), yi, y_peers)
    late = jnp.sum(collect(3, late_y, yi), axis=1, keepdims=True)
    g_ahead, g_behind, g_g, energy = (
        jnp.broadcast_to(late[k : k + 1], (1, 128)) for k in range(4)
    )
    along = (g_ahead / len_ahead + g_behind / len_behind) / raw_len
    count = float(chain_n)
    goal = (ci + 1).astype(F32) / (count + 1.0) * band
    climbing = climb_ref[:, 0:1] == 1
    coef = jnp.where(climbing, 2.0 * along, along + SPRING * (goal - arc) / band)
    force_sq = g_g - 2.0 * coef * along + coef * coef * tau_sq
    scale = band / (count + 1.0) / jnp.sqrt(force_sq + EPS)
    wa = (scale * coef / (len_ahead * raw_len))[:, 0:1]
    wb = (scale * coef / (len_behind * raw_len))[:, 0:1]
    scale = scale[:, 0:1]
    for m, up in enumerate((up_in, up_mid, up_out)):
        n = up.shape[1]
        u = wa * AH[m, :, :n] + wb * BH[m, :, :n] - scale * gsh[m, :, :n]
        up[...] = own[m][...] + u
    tab_ref[...] = pack(0.5 * norm * energy, arc / band, 0.5 * raw_len)
    for c in cp.all:
        c.wait_send()


def on_device(
    images_in, images_mid, images_out, ends_in, ends_mid, ends_out, data_pool, batch_rows, labels, climbing
):
    _, shard, hidden_units = images_in.shape
    width = data_pool.shape[1]
    classes = images_out.shape[2]
    rows = batch_rows.shape[1]
    pool_rows = data_pool.shape[0]
    chain_n = lax.axis_size("chain")
    batch = rows * lax.axis_size(DP)
    any_spec = pl.BlockSpec(memory_space=pl.ANY)
    vmem_spec = pl.BlockSpec(memory_space=pltpu.VMEM)
    vm = pltpu.VMEM
    scratch = [
        vm((3, SIDE, SIDE, 2, 32, width), BF16),
        vm((3, SIDE, SIDE, 2, 32, width), BF16),
        vm((3, 2, 2, 2, 32, width), BF16),
        vm((3, 2, 2, 2, 32, width), BF16),
        vm((3, 2, 2, 2, 32, width), BF16),
        vm((3, 2, SIDE, 32, width), BF16),
        vm((3, 2, 2, 16, width), BF16),
        vm((3, 2, 2, 16, width), BF16),
        vm((3, 2, 2, 16, width), BF16),
        vm((3, shard, width), F32),
        vm((shard, width), F32),
        vm((shard, width), F32),
        vm((shard, classes), F32),
        vm((2, shard, width), F32),
        vm((2, shard, width), F32),
        vm((2, shard, classes), F32),
        vm((2, shard, width), F32),
        vm((2, shard, width), F32),
        vm((2, shard, classes), F32),
        vm((3, shard, width), F32),
        vm((3, shard, width), F32),
        vm((pool_rows, width), BF16),
        vm((rows, pool_rows), BF16),
        vm((rows, 128), F32),
        vm((rows, 128), F32),
        vm((rows, width), BF16),
        vm((rows, width), BF16),
        vm((rows, width), F32),
        vm((rows, width), BF16),
        vm((rows, width), BF16),
        vm((rows, width), BF16),
        vm((rows, width), BF16),
        vm((4, 8, 128), F32),
        vm((4, SIDE, 8, 128), F32),
        vm((8, 128), F32),
        vm((chain_n, 8, 128), F32),
        pltpu.SemaphoreType.DMA((7,)),
        pltpu.SemaphoreType.DMA((N_COPIES,)),
        pltpu.SemaphoreType.DMA((N_COPIES,)),
    ]
    climb = jnp.broadcast_to(climbing[:, None], (1, 128))
    up_in, up_mid, up_out, tab = pl.pallas_call(
        functools.partial(kernel, (chain_n, batch, classes)),
        out_shape=(
            jax.ShapeDtypeStruct((shard, hidden_units), F32),
            jax.ShapeDtypeStruct((shard, width), F32),
            jax.ShapeDtypeStruct((shard, classes), F32),
            jax.ShapeDtypeStruct((8, 128), F32),
        ),
        in_specs=[any_spec] * 7 + [vmem_spec] * 3,
        out_specs=(vmem_spec,) * 4,
        scratch_shapes=scratch,
        compiler_params=pltpu.CompilerParams(
            collective_id=0, has_side_effects=True, vmem_limit_bytes=60 * 2**20
        ),
        cost_estimate=pl.CostEstimate(
            flops=2 * rows * width * (8 * width + pool_rows), bytes_accessed=10**7, transcendentals=10**6
        ),
        name="band_step",
    )(images_in, images_mid, images_out, ends_in, ends_mid, ends_out, data_pool, batch_rows, labels, climb)
    return (up_in[None], up_mid[None], up_out[None], tab[0, 0:1], tab[1, 0:1], tab[2, 0:1])


def solution(mesh):
    torus = Mesh(mesh.devices.reshape(mesh.shape["chain"], SIDE, SIDE), ("chain", "dp_0", "dp_1"))
    shard = P("chain", DP, None)
    end = P(None, DP, None)
    in_specs = (
        shard, shard, shard, end, end, end, P(DP, None), P("chain", DP), P("chain", DP), P("chain"),
    )
    out_specs = (shard, shard, shard, P("chain"), P("chain"), P("chain"))
    return jax.shard_map(
        on_device, mesh=torus, in_specs=in_specs, out_specs=out_specs, check_vma=False
    )
```

```python
import functools

import jax
import jax.numpy as jnp
from jax import lax
from jax.experimental import pallas as pl
from jax.experimental.pallas import tpu as pltpu
from jax.sharding import Mesh
from jax.sharding import PartitionSpec as P

DP = ("dp_0", "dp_1")
SPRING = 0.03
EPS = 1e-06
F32 = jnp.float32
BF16 = jnp.bfloat16
SIDE = 4
N_COPIES = 280


def mm(a, b):
    return jnp.dot(a, b, preferred_element_type=F32)


def mm_nt(a, b):
    return lax.dot_general(a, b, (((1,), (1,)), ((), ())), preferred_element_type=F32)


def mm_tn(a, b):
    return lax.dot_general(a, b, (((0,), (0,)), ((), ())), preferred_element_type=F32)


class Copies:
    def __init__(self, send, recv):
        self.send, self.recv, self.all = send, recv, []

    def start(self, src, dst, device):
        i = len(self.all)
        copy = pltpu.make_async_remote_copy(
            src_ref=src,
            dst_ref=dst,
            send_sem=self.send.at[i],
            recv_sem=self.recv.at[i],
            device_id=device,
            device_id_type=pl.DeviceIdType.MESH,
        )
        copy.start()
        self.all.append(copy)
        return copy


def kernel(
    dims,
    im_in, im_mid, im_out, en_in, en_mid, en_out, pool_hbm, rows_hbm, labs_hbm, climb_hbm,
    up_in, up_mid, up_out, tab_ref,
    W, G, RA1, RAd, RAs, R1, RB1, RBd, RBs, gsh,
    own_in, own_mid, own_out, nb_in, nb_mid, nb_out, e_in, e_mid, e_out, AH, BH,
    pool, onehot, rcol, lcol, x, hid, slope, resid, dlog, dres, dpre,
    rows_ref, labs_ref, climb_ref, mine, sums, chain_tab,
    local_sem, send_sem, recv_sem,
):
    chain_n, batch, classes = dims
    rows = x.shape[0]
    width = x.shape[1]
    half_rows = rows // 2
    ci = lax.axis_index("chain")
    yi = lax.axis_index("dp_0")
    xi = lax.axis_index("dp_1")
    cp = Copies(send_sem, recv_sem)

    def at_x(step):
        return {"dp_1": lax.rem(xi + step, SIDE)}

    def at_y(step):
        return {"dp_0": lax.rem(yi + step, SIDE)}

    def xs(step):
        return lax.rem(xi + step, SIDE)

    def ys(step):
        return lax.rem(yi + step, SIDE)

    def at_chain(step):
        return {"chain": lax.rem(ci + step, chain_n)}

    barrier = pltpu.get_barrier_semaphore()
    partners = [at_x(1), at_x(3), at_y(1), at_y(3), at_chain(1), at_chain(chain_n - 1)]
    for device in partners:
        pl.semaphore_signal(barrier, inc=1, device_id=device, device_id_type=pl.DeviceIdType.MESH)

    loads = []

    def load(src, dst):
        c = pltpu.make_async_copy(src, dst, local_sem.at[len(loads)])
        c.start()
        loads.append(c)

    load(im_in.at[0], own_in)
    load(im_mid.at[0], own_mid)
    load(im_out.at[0], own_out)
    load(pool_hbm, pool)
    load(rows_hbm, rows_ref)
    load(labs_hbm, labs_ref)
    load(climb_hbm, climb_ref)
    load(en_in, e_in)
    load(en_mid, e_mid)
    load(en_out, e_out)

    factors = (width ** (-0.5), hid.shape[1] ** (-0.5), width ** (-0.5))
    edge = classes // 128 * 128
    for m, ref in enumerate((own_in, own_mid, own_out)):
        loads[m].wait()
        if m == 2:
            W[m, yi, xi, :, :, edge:] = jnp.zeros((2, 32, width - edge), BF16)
        n = ref.shape[1]
        W[m, yi, xi, :, :, :n] = (ref[...] * factors[m]).astype(BF16).reshape(2, 32, n)
    pl.semaphore_wait(barrier, len(partners))

    DIRS = (1, 3)

    def near(h, d):
        return at_x(d) if h == 0 else at_y(d)

    def far(h, d):
        return at_y(d) if h == 0 else at_x(d)

    def piece(m, h, far_step, near_step, k=None):
        r = pl.ds(0, 32) if k is None else pl.ds(16 * k, 16)
        if h == 0:
            return W.at[m, ys(far_step), xs(near_step), h, r]
        return W.at[m, ys(near_step), xs(far_step), h, r]

    def blocks(ref, m, h, step, k, cols=None):
        two = pl.ds(2 * k, 2)
        cols = pl.ds(0, ref.shape[-1]) if cols is None else cols
        if h == 0:
            return ref.at[m, ys(step), two, 0, :, cols]
        return ref.at[m, two, xs(step), 1, :, cols]

    BOTH = [(h, k) for h in (0, 1) for k in (0, 1)]
    ALL = pl.ds(0, 3)
    near_one, near_fwd, own_far, own_fwd, far_one, far_fwd = {}, {}, {}, {}, {}, {}
    for h, k in BOTH:
        src = piece(ALL, h, 0, 0)
        near_one[h, k] = cp.start(src, src, near(h, DIRS[k]))
    for h, k in BOTH:
        src = piece(ALL, h, 0, 0)
        own_far[h, k] = cp.start(src, src, far(h, DIRS[k]))

    nb = []
    for own, buf in ((own_in, nb_in), (own_mid, nb_mid), (own_out, nb_out)):
        nb.append(cp.start(own, buf.at[0], at_chain(1)))
        nb.append(cp.start(own, buf.at[1], at_chain(chain_n - 1)))

    def ag_near_forward():
        for h, k in BOTH:
            near_one[h, k].wait_recv()
            src = piece(ALL, h, 0, SIDE - DIRS[k], k)
            near_fwd[h, k] = cp.start(src, src, near(h, DIRS[k]))

    def ag_far(m, steps):
        for j in steps:
            for h, k in BOTH:
                src = piece(m, h, 0, j)
                far_one[m, h, k, j] = cp.start(src, src, far(h, DIRS[k]))

    def ag_own_forward():
        for h, k in BOTH:
            own_far[h, k].wait_recv()
            src = piece(ALL, h, SIDE - DIRS[k], 0, k)
            own_fwd[h, k] = cp.start(src, src, far(h, DIRS[k]))

    def ag_near_end():
        for h, k in BOTH:
            near_fwd[h, k].wait_recv()

    def ag_far_forward(m, steps):
        for j in steps:
            for h, k in BOTH:
                far_one[m, h, k, j].wait_recv()
                src = piece(m, h, SIDE - DIRS[k], j, k)
                far_fwd[m, h, k, j] = cp.start(src, src, far(h, DIRS[k]))

    def ag_end(m):
        for h, k in BOTH:
            if m == 0:
                own_fwd[h, k].wait_recv()
            for j in (1, 2, 3):
                far_fwd[m, h, k, j].wait_recv()

    def weight(m):
        return W[m].reshape(width, width)

    def part(i):
        return pl.ds(i * half_rows, half_rows)

    SIDES, ACROSS = (1, 3), (2,)

    for c in loads[4:7]:
        c.wait()
    for ref, col in ((rows_ref, rcol), (labs_ref, lcol)):
        for k in range(rows // 128):
            r = pl.ds(k * 128, 128)
            col[r, :] = jnp.transpose(jnp.broadcast_to(ref[:, r].astype(F32), (128, 128)))

    def lanes(c):
        return (lax.broadcasted_iota(jnp.int32, (1, 128), 1) + 128 * c).astype(F32)

    def pick_rows(i):
        for c in range(pool.shape[0] // 128):
            hit = rcol[part(i), :] == lanes(c)
            onehot[part(i), c * 128 : (c + 1) * 128] = jnp.where(hit, 1.0, 0.0).astype(BF16)
        x[part(i), :] = mm(onehot[part(i), :], pool[...]).astype(BF16)

    loads[3].wait()
    pick_rows(0)
    ag_near_forward()
    ag_far(0, SIDES)
    pick_rows(1)
    ag_own_forward()

    for c in loads[7:]:
        c.wait()
    for c in nb:
        c.wait_recv()
    first, last = ci == 0, ci == chain_n - 1
    own = (own_in, own_mid, own_out)
    sq_a = sq_b = cross = jnp.zeros((1, 128), F32)

    def fold(v):
        v = jnp.sum(v, axis=0, keepdims=True)
        out = v[:, :128]
        for c in range(1, v.shape[1] // 128):
            out = out + v[:, c * 128 : (c + 1) * 128]
        return out

    for m, (e, b) in enumerate(((e_in, nb_in), (e_mid, nb_mid), (e_out, nb_out))):
        n = own[m].shape[1]
        o = own[m][...]
        if m == 2:
            AH[m, :, edge:] = jnp.zeros((o.shape[0], width - edge), F32)
            BH[m, :, edge:] = jnp.zeros((o.shape[0], width - edge), F32)
        AH[m, :, :n] = jnp.where(last, e[1], b[1]) - o
        BH[m, :, :n] = o - jnp.where(first, e[0], b[0])
        a, z = AH[m], BH[m]
        sq_a, sq_b, cross = sq_a + fold(a * a), sq_b + fold(z * z), cross + fold(a * z)

    def pack(*values):
        zero = jnp.zeros((8 - len(values), 128), F32)
        return jnp.concatenate([*values, zero], axis=0)

    def exchange(slot, tile, index, peers):
        mine[slot] = tile
        return [cp.start(mine.at[slot], sums.at[slot, index], device) for device in peers]

    def collect(slot, copies, index):
        for c in copies:
            c.wait_recv()
        sums[slot, index] = mine[slot]
        out = sums[slot, 0]
        for k in range(1, SIDE):
            out = out + sums[slot, k]
        return out

    x_peers = [at_x(s) for s in (1, 2, 3)]
    y_peers = [at_y(s) for s in (1, 2, 3)]
    early_x = exchange(0, pack(sq_b, sq_a, cross), xi, x_peers)
    ag_near_end()
    ag_far(0, ACROSS)
    ag_far(1, SIDES)
    ag_far_forward(0, SIDES)
    early_y = exchange(1, collect(0, early_x, xi), yi, y_peers)
    ag_far_forward(0, ACROSS)
    ag_far(1, ACROSS)
    ag_far(2, SIDES)
    early = jnp.sum(collect(1, early_y, yi), axis=1, keepdims=True)
    sq_behind = jnp.broadcast_to(early[0:1], (1, 128))
    sq_ahead = jnp.broadcast_to(early[1:2], (1, 128))
    cross = jnp.broadcast_to(early[2:3], (1, 128))
    len_ahead = jnp.sqrt(sq_ahead + EPS)
    len_behind = jnp.sqrt(sq_behind + EPS)
    raw_sq = (
        sq_ahead / (len_ahead * len_ahead)
        + sq_behind / (len_behind * len_behind)
        + 2.0 * cross / (len_ahead * len_behind)
    )
    raw_len = jnp.sqrt(raw_sq + EPS)
    tau_sq = raw_sq / (raw_sq + EPS)
    chain_tab[ci] = pack(len_behind, len_ahead)
    up, down = {}, {}

    def lengths(step):
        if step > 1:
            up[step - 1].wait_recv()
        if step <= chain_n // 2:
            src = chain_tab.at[lax.rem(ci + chain_n + 1 - step, chain_n)]
            up[step] = cp.start(src, src, at_chain(1))
        if 1 < step <= chain_n // 2:
            down[step - 1].wait_recv()
        if step < chain_n // 2:
            src = chain_tab.at[lax.rem(ci + step - 1, chain_n)]
            down[step] = cp.start(src, src, at_chain(chain_n - 1))

    lengths(1)

    def forward_in(i):
        pre = mm(x[part(i), :], weight(0))
        sig = jax.nn.sigmoid(pre)
        hid[part(i), :] = (pre * sig).astype(BF16)
        slope[part(i), :] = sig * (1.0 + pre * (1.0 - sig))

    def forward_mid(i):
        r = x[part(i), :].astype(F32) + mm(hid[part(i), :], weight(1))
        resid[part(i), :] = r.astype(BF16)

    norm = 1.0 / (batch * classes)

    COLS = width // 2

    def cols_of(c):
        return pl.ds(c * COLS, COLS)

    def forward_out(i, energy):
        logits = mm(resid[...], W[2, :, :, :, :, cols_of(i)].reshape(width, COLS))
        for c in range(COLS // 128):
            at = i * COLS + c * 128
            hit = lcol[...] == lanes(i * (COLS // 128) + c)
            err = logits[:, c * 128 : (c + 1) * 128] - jnp.where(hit, 1.0, 0.0)
            energy = energy + jnp.sum(err * err, axis=0, keepdims=True)
            dlog[:, at : at + 128] = (err * norm).astype(BF16)
        return energy

    ag_far_forward(1, SIDES)
    ag_end(0)
    forward_in(0)
    ag_far_forward(1, ACROSS)
    ag_far(2, ACROSS)
    lengths(2)
    forward_in(1)
    ag_far_forward(2, SIDES)
    lengths(3)
    ag_end(1)
    forward_mid(0)
    ag_far_forward(2, ACROSS)
    lengths(4)
    forward_mid(1)
    ag_end(2)

    PIECES = [(m, c) for m in (2, 1, 0) for c in (0, 1)]

    def grad(p, left, right):
        m, c = PIECES[p]
        g = mm_tn(left[...], right[:, cols_of(c)]).astype(BF16)
        G[m, :, :, :, :, cols_of(c)] = g.reshape(SIDE, SIDE, 2, 32, COLS)

    a1, ad, a_s, b1, bd, bs = {}, {}, {}, {}, {}, {}

    def rs_start(p):
        m, c = PIECES[p]
        q = cols_of(c)
        for h, k in BOTH:
            dst = RA1.at[m, h, k, :, :, q]
            a1[p, h, k] = cp.start(blocks(G, m, h, 2, k, q), dst, far(h, DIRS[k]))
        for h, k in BOTH:
            dst = RAd.at[m, h, k, :, :, q]
            src = blocks(G, m, h, DIRS[k], 1 - k, q)
            ad[p, h, k] = cp.start(src, dst, far(h, DIRS[k]))

    def rs_far_sum(p):
        m, c = PIECES[p]
        q = cols_of(c)
        for h, k in BOTH:
            a1[p, h, k].wait_recv()
            mid = RA1.at[m, h, k, :, :, q]
            own_g = blocks(G, m, h, DIRS[k], k, q)
            mid[...] = (mid[...].astype(F32) + own_g[...].astype(F32)).astype(BF16)
            a_s[p, h, k] = cp.start(mid, RAs.at[m, h, k, :, :, q], far(h, DIRS[k]))

    def rs_near_start(p):
        m, c = PIECES[p]
        q = cols_of(c)
        for h in (0, 1):
            for k in (0, 1):
                ad[p, h, k].wait_recv()
                a_s[p, h, k].wait_recv()
            for k in (0, 1):
                total = blocks(G, m, h, 0, k, q)[...].astype(F32)
                total = total + RAs[m, h, k, :, :, q].astype(F32)
                total = total + RAd[m, h, 1 - k, :, :, q].astype(F32)
                R1[m, h, pl.ds(2 * k, 2), :, q] = total.astype(BF16)
            for k in (0, 1):
                step = ys if h else xs
                src = R1.at[m, h, step(2), pl.ds(16 * k, 16), q]
                b1[p, h, k] = cp.start(src, RB1.at[m, h, k, :, q], near(h, DIRS[k]))
            for k in (0, 1):
                src = R1.at[m, h, step(DIRS[k]), pl.ds(16 * (1 - k), 16), q]
                bd[p, h, k] = cp.start(src, RBd.at[m, h, k, :, q], near(h, DIRS[k]))

    def rs_near_sum(p):
        m, c = PIECES[p]
        q = cols_of(c)
        for h, k in BOTH:
            step = ys if h else xs
            b1[p, h, k].wait_recv()
            mid = RB1.at[m, h, k, :, q]
            own_r = R1[m, h, step(DIRS[k]), pl.ds(16 * k, 16), q]
            mid[...] = (mid[...].astype(F32) + own_r.astype(F32)).astype(BF16)
            bs[p, h, k] = cp.start(mid, RBs.at[m, h, k, :, q], near(h, DIRS[k]))

    dots = [jnp.zeros((1, 128), F32)] * 3

    def rs_end(p):
        m, c = PIECES[p]
        q = cols_of(c)
        for h in (0, 1):
            step = ys if h else xs
            for k in (0, 1):
                bd[p, h, k].wait_recv()
                bs[p, h, k].wait_recv()
            for k in (0, 1):
                total = R1[m, h, step(0), pl.ds(16 * k, 16), q].astype(F32)
                total = total + RBs[m, h, k, :, q].astype(F32)
                total = total + RBd[m, h, 1 - k, :, q].astype(F32)
                g = total * factors[m]
                r = pl.ds(32 * h + 16 * k, 16)
                gsh[m, r, q] = g
                dots[0] = dots[0] + fold(g * AH[m, r, q])
                dots[1] = dots[1] + fold(g * BH[m, r, q])
                dots[2] = dots[2] + fold(g * g)

    def back_resid(i):
        dres[part(i), :] = mm_nt(dlog[part(i), :], weight(2)).astype(BF16)

    def back_pre(i):
        d = mm_nt(dres[part(i), :], weight(1)) * slope[part(i), :]
        dpre[part(i), :] = d.astype(BF16)

    energy = forward_out(0, jnp.zeros((1, 128), F32))
    grad(0, resid, dlog)
    rs_start(0)
    energy = forward_out(1, energy)
    grad(1, resid, dlog)
    rs_start(1)
    back_resid(0)
    rs_far_sum(0)
    lengths(5)
    back_resid(1)
    rs_far_sum(1)
    lengths(6)
    grad(2, hid, dres)
    rs_start(2)
    grad(3, hid, dres)
    rs_start(3)
    back_pre(0)
    rs_far_sum(2)
    lengths(7)
    back_pre(1)
    grad(4, x, dpre)
    rs_start(4)
    rs_far_sum(3)
    lengths(8)
    grad(5, x, dpre)
    rs_start(5)
    rs_near_start(0)
    rs_far_sum(4)
    rs_near_start(1)
    rs_far_sum(5)
    rs_near_start(2)
    lengths(9)
    arc = jnp.zeros((1, 128), F32)
    band = jnp.zeros((1, 128), F32)
    for j in range(chain_n):
        length = chain_tab[j, 0:1]
        arc = arc + jnp.where(j <= ci, length, 0.0)
        band = band + length
    band = band + chain_tab[chain_n - 1, 1:2]
    rs_near_sum(0)
    rs_near_start(3)
    rs_near_sum(1)
    rs_near_start(4)
    rs_near_sum(2)
    rs_near_start(5)
    rs_near_sum(3)
    rs_end(0)
    rs_end(1)
    rs_near_sum(4)
    rs_end(2)
    rs_near_sum(5)
    rs_end(3)
    rs_end(4)
    rs_end(5)

    late_x = exchange(2, pack(*dots, energy), xi, x_peers)
    late_y = exchange(3, collect(2, late_x, xi), yi, y_peers)
    late = jnp.sum(collect(3, late_y, yi), axis=1, keepdims=True)
    g_ahead, g_behind, g_g, energy = (
        jnp.broadcast_to(late[k : k + 1], (1, 128)) for k in range(4)
    )
    along = (g_ahead / len_ahead + g_behind / len_behind) / raw_len
    count = float(chain_n)
    goal = (ci + 1).astype(F32) / (count + 1.0) * band
    climbing = jnp.full((1, 128), climb_ref[0]) == 1
    coef = jnp.where(climbing, 2.0 * along, along + SPRING * (goal - arc) / band)
    force_sq = g_g - 2.0 * coef * along + coef * coef * tau_sq
    scale = band / (count + 1.0) / jnp.sqrt(force_sq + EPS)
    wa = (scale * coef / (len_ahead * raw_len))[:, 0:1]
    wb = (scale * coef / (len_behind * raw_len))[:, 0:1]
    scale = scale[:, 0:1]
    for m, up in enumerate((up_in, up_mid, up_out)):
        n = up.shape[1]
        u = wa * AH[m, :, :n] + wb * BH[m, :, :n] - scale * gsh[m, :, :n]
        up[...] = own[m][...] + u
    tab_ref[...] = pack(0.5 * norm * energy, arc / band, 0.5 * raw_len)
    for c in cp.all:
        c.wait_send()


def hand_out(up_in, up_mid, up_out, tab, new_in, new_mid, new_out, energy, share, bend):
    for up, new in ((up_in, new_in), (up_mid, new_mid), (up_out, new_out)):
        new[0] = up[...]
    energy[0], share[0], bend[0] = tab[0, 0], tab[1, 0], tab[2, 0]


def on_device(
    images_in, images_mid, images_out, ends_in, ends_mid, ends_out, data_pool, batch_rows, labels, climbing
):
    _, shard, hidden_units = images_in.shape
    width = data_pool.shape[1]
    classes = images_out.shape[2]
    rows = batch_rows.shape[1]
    pool_rows = data_pool.shape[0]
    chain_n = lax.axis_size("chain")
    batch = rows * lax.axis_size(DP)
    any_spec = pl.BlockSpec(memory_space=pl.ANY)
    vmem_spec = pl.BlockSpec(memory_space=pltpu.VMEM)
    vm = pltpu.VMEM
    scratch = [
        vm((3, SIDE, SIDE, 2, 32, width), BF16),
        vm((3, SIDE, SIDE, 2, 32, width), BF16),
        vm((3, 2, 2, 2, 32, width), BF16),
        vm((3, 2, 2, 2, 32, width), BF16),
        vm((3, 2, 2, 2, 32, width), BF16),
        vm((3, 2, SIDE, 32, width), BF16),
        vm((3, 2, 2, 16, width), BF16),
        vm((3, 2, 2, 16, width), BF16),
        vm((3, 2, 2, 16, width), BF16),
        vm((3, shard, width), F32),
        vm((shard, width), F32),
        vm((shard, width), F32),
        vm((shard, classes), F32),
        vm((2, shard, width), F32),
        vm((2, shard, width), F32),
        vm((2, shard, classes), F32),
        vm((2, shard, width), F32),
        vm((2, shard, width), F32),
        vm((2, shard, classes), F32),
        vm((3, shard, width), F32),
        vm((3, shard, width), F32),
        vm((pool_rows, width), BF16),
        vm((rows, pool_rows), BF16),
        vm((rows, 128), F32),
        vm((rows, 128), F32),
        vm((rows, width), BF16),
        vm((rows, width), BF16),
        vm((rows, width), F32),
        vm((rows, width), BF16),
        vm((rows, width), BF16),
        vm((rows, width), BF16),
        vm((rows, width), BF16),
        vm((1, rows), jnp.int32),
        vm((1, rows), jnp.int32),
        pltpu.SMEM((1,), jnp.int32),
        vm((4, 8, 128), F32),
        vm((4, SIDE, 8, 128), F32),
        vm((chain_n, 8, 128), F32),
        pltpu.SemaphoreType.DMA((10,)),
        pltpu.SemaphoreType.DMA((N_COPIES,)),
        pltpu.SemaphoreType.DMA((N_COPIES,)),
    ]
    up_in, up_mid, up_out, tab = pl.pallas_call(
        functools.partial(kernel, (chain_n, batch, classes)),
        out_shape=(
            jax.ShapeDtypeStruct((shard, hidden_units), F32),
            jax.ShapeDtypeStruct((shard, width), F32),
            jax.ShapeDtypeStruct((shard, classes), F32),
            jax.ShapeDtypeStruct((8, 128), F32),
        ),
        in_specs=[any_spec] * 9 + [pl.BlockSpec(memory_space=pltpu.HBM)],
        out_specs=(vmem_spec,) * 4,
        scratch_shapes=scratch,
        compiler_params=pltpu.CompilerParams(
            collective_id=0, has_side_effects=True, vmem_limit_bytes=56 * 2**20
        ),
        cost_estimate=pl.CostEstimate(
            flops=2 * rows * width * (8 * width + pool_rows), bytes_accessed=10**7, transcendentals=10**6
        ),
        name="band_step",
    )(images_in, images_mid, images_out, ends_in, ends_mid, ends_out, data_pool, batch_rows, labels, climbing)
    scalar = jax.ShapeDtypeStruct((1,), F32)
    smem_spec = pl.BlockSpec(memory_space=pltpu.SMEM)
    return pl.pallas_call(
        hand_out,
        out_shape=(
            jax.ShapeDtypeStruct(images_in.shape, F32),
            jax.ShapeDtypeStruct(images_mid.shape, F32),
            jax.ShapeDtypeStruct(images_out.shape, F32),
            scalar,
            scalar,
            scalar,
        ),
        in_specs=[vmem_spec] * 3 + [smem_spec],
        out_specs=(vmem_spec,) * 3 + (smem_spec,) * 3,
        name="hand_out",
    )(up_in, up_mid, up_out, tab)


def solution(mesh):
    torus = Mesh(mesh.devices.reshape(mesh.shape["chain"], SIDE, SIDE), ("chain", "dp_0", "dp_1"))
    shard = P("chain", DP, None)
    end = P(None, DP, None)
    in_specs = (
        shard, shard, shard, end, end, end, P(DP, None), P("chain", DP), P("chain", DP), P("chain"),
    )
    out_specs = (shard, shard, shard, P("chain"), P("chain"), P("chain"))
    return jax.shard_map(
        on_device, mesh=torus, in_specs=in_specs, out_specs=out_specs, check_vma=False
    )
```

```python
import functools

import jax
import jax.numpy as jnp
from jax import lax
from jax.experimental import pallas as pl
from jax.experimental.pallas import tpu as pltpu
from jax.sharding import Mesh
from jax.sharding import PartitionSpec as P

DP = ("dp_0", "dp_1")
SPRING = 0.03
EPS = 1e-06
F32 = jnp.float32
BF16 = jnp.bfloat16
SIDE = 4
N_COPIES = 64


def mm(a, b):
    return jnp.dot(a, b, preferred_element_type=F32)


def mm_nt(a, b):
    return lax.dot_general(a, b, (((1,), (1,)), ((), ())), preferred_element_type=F32)


def mm_tn(a, b):
    return lax.dot_general(a, b, (((0,), (0,)), ((), ())), preferred_element_type=F32)


class Group:
    def __init__(self, copies, whole):
        i = len(copies.all)
        self.sems = (copies.send.at[i], copies.recv.at[i])
        self.whole = whole
        copies.all.append(self)

    def _copy(self, src, dst, device):
        return pltpu.make_async_remote_copy(
            src_ref=src,
            dst_ref=dst,
            send_sem=self.sems[0],
            recv_sem=self.sems[1],
            device_id=device,
            device_id_type=pl.DeviceIdType.MESH,
        )

    def start(self, src, dst, device):
        self.device = device
        self._copy(src, dst, device).start()

    def wait_recv(self):
        self._copy(self.whole, self.whole, self.device).wait_recv()

    def wait_send(self):
        self._copy(self.whole, self.whole, self.device).wait_send()


class Copies:
    def __init__(self, send, recv):
        self.send, self.recv, self.all = send, recv, []

    def group(self, whole):
        return Group(self, whole)


def kernel(
    dims,
    im_in, im_mid, im_out, en_in, en_mid, en_out, pool_hbm, rows_hbm, labs_hbm, climb_hbm,
    up_in, up_mid, up_out, tab_ref,
    W, G, RA1, RAd, RAs, R1, RB1, RBd, RBs, gsh,
    own_in, own_mid, own_out, nb_in, nb_mid, nb_out, e_in, e_mid, e_out, AH, BH,
    pool, onehot, rcol, lcol, x, hid, slope, resid, dlog, dres, dpre,
    rows_ref, labs_ref, climb_ref, sums, chain_tab, out_in, out_mid, out_out, out_tab,
    local_sem, send_sem, recv_sem,
):
    chain_n, batch, classes = dims
    rows = x.shape[0]
    width = x.shape[1]
    half_rows = rows // 2
    ci = lax.axis_index("chain")
    yi = lax.axis_index("dp_0")
    xi = lax.axis_index("dp_1")
    cp = Copies(send_sem, recv_sem)

    def at_x(step):
        return {"dp_1": lax.rem(xi + step, SIDE)}

    def at_y(step):
        return {"dp_0": lax.rem(yi + step, SIDE)}

    def xs(step):
        return lax.rem(xi + step, SIDE)

    def ys(step):
        return lax.rem(yi + step, SIDE)

    def at_chain(step):
        return {"chain": lax.rem(ci + step, chain_n)}

    barrier = pltpu.get_barrier_semaphore()
    partners = [at_x(1), at_x(3), at_y(1), at_y(3), at_chain(1), at_chain(chain_n - 1)]
    for device in partners:
        pl.semaphore_signal(barrier, inc=1, device_id=device, device_id_type=pl.DeviceIdType.MESH)

    loads = []

    def load(src, dst):
        c = pltpu.make_async_copy(src, dst, local_sem.at[len(loads)])
        c.start()
        loads.append(c)

    load(im_in.at[0], own_in)
    load(im_mid.at[0], own_mid)
    load(im_out.at[0], own_out)
    load(pool_hbm, pool)
    load(rows_hbm, rows_ref)
    load(labs_hbm, labs_ref)
    load(climb_hbm, climb_ref)
    load(en_in, e_in)
    load(en_mid, e_mid)
    load(en_out, e_out)

    factors = (width ** (-0.5), hid.shape[1] ** (-0.5), width ** (-0.5))
    edge = classes // 128 * 128
    for m, ref in enumerate((own_in, own_mid, own_out)):
        loads[m].wait()
        if m == 2:
            W[m, yi, xi, :, :, edge:] = jnp.zeros((2, 32, width - edge), BF16)
        n = ref.shape[1]
        W[m, yi, xi, :, :, :n] = (ref[...] * factors[m]).astype(BF16).reshape(2, 32, n)
    pl.semaphore_wait(barrier, len(partners))

    DIRS = (1, 3)

    def near(h, d):
        return at_x(d) if h == 0 else at_y(d)

    def far(h, d):
        return at_y(d) if h == 0 else at_x(d)

    def piece(m, h, far_step, near_step, k=None):
        r = pl.ds(0, 32) if k is None else pl.ds(16 * k, 16)
        if h == 0:
            return W.at[m, ys(far_step), xs(near_step), h, r]
        return W.at[m, ys(near_step), xs(far_step), h, r]

    def blocks(ref, m, h, step, k, cols=None):
        two = pl.ds(2 * k, 2)
        cols = pl.ds(0, ref.shape[-1]) if cols is None else cols
        if h == 0:
            return ref.at[m, ys(step), two, 0, :, cols]
        return ref.at[m, two, xs(step), 1, :, cols]

    BOTH = [(h, k) for h in (0, 1) for k in (0, 1)]
    ALL = pl.ds(0, 3)
    near_one = cp.group(W.at[ALL, 0, :, 0])
    own_far = cp.group(W.at[ALL, 0, :, 0])
    far_one, far_fwd = {}, {}
    for h, k in BOTH:
        src = piece(ALL, h, 0, 0)
        near_one.start(src, src, near(h, DIRS[k]))
    for h, k in BOTH:
        src = piece(ALL, h, 0, 0)
        own_far.start(src, src, far(h, DIRS[k]))

    nb = []
    for own, buf in ((own_in, nb_in), (own_mid, nb_mid), (own_out, nb_out)):
        nb.append(cp.group(buf))
        nb[-1].start(own, buf.at[0], at_chain(1))
        nb[-1].start(own, buf.at[1], at_chain(chain_n - 1))

    near_fwd = cp.group(W.at[ALL, 0, pl.ds(0, 2), 0])
    own_fwd = cp.group(W.at[ALL, 0, pl.ds(0, 2), 0])

    def ag_near_forward():
        near_one.wait_recv()
        for h, k in BOTH:
            src = piece(ALL, h, 0, SIDE - DIRS[k], k)
            near_fwd.start(src, src, near(h, DIRS[k]))

    def ag_far(m, steps):
        far_one[m, steps] = cp.group(W.at[m, pl.ds(0, len(steps)), :, 0])
        for j in steps:
            for h, k in BOTH:
                src = piece(m, h, 0, j)
                far_one[m, steps].start(src, src, far(h, DIRS[k]))

    def ag_own_forward():
        own_far.wait_recv()
        for h, k in BOTH:
            src = piece(ALL, h, SIDE - DIRS[k], 0, k)
            own_fwd.start(src, src, far(h, DIRS[k]))

    def ag_near_end():
        near_fwd.wait_recv()

    def ag_far_forward(m, steps):
        far_one[m, steps].wait_recv()
        far_fwd[m, steps] = cp.group(W.at[m, 0, pl.ds(0, 2 * len(steps)), 0])
        for j in steps:
            for h, k in BOTH:
                src = piece(m, h, SIDE - DIRS[k], j, k)
                far_fwd[m, steps].start(src, src, far(h, DIRS[k]))

    def ag_end(m):
        if m == 0:
            own_fwd.wait_recv()
        far_fwd[m, SIDES].wait_recv()
        far_fwd[m, ACROSS].wait_recv()

    def weight(m):
        return W[m].reshape(width, width)

    def part(i):
        return pl.ds(i * half_rows, half_rows)

    SIDES, ACROSS = (1, 3), (2,)

    for c in loads[4:7]:
        c.wait()
    for ref, col in ((rows_ref, rcol), (labs_ref, lcol)):
        for k in range(rows // 128):
            r = pl.ds(k * 128, 128)
            col[r, :] = jnp.transpose(jnp.broadcast_to(ref[:, r].astype(F32), (128, 128)))

    def lanes(c):
        return (lax.broadcasted_iota(jnp.int32, (1, 128), 1) + 128 * c).astype(F32)

    def pick_rows(i):
        for c in range(pool.shape[0] // 128):
            hit = rcol[part(i), :] == lanes(c)
            onehot[part(i), c * 128 : (c + 1) * 128] = jnp.where(hit, 1.0, 0.0).astype(BF16)
        x[part(i), :] = mm(onehot[part(i), :], pool[...]).astype(BF16)

    loads[3].wait()
    pick_rows(0)
    ag_near_forward()
    ag_far(0, SIDES)
    pick_rows(1)
    ag_own_forward()

    for c in loads[7:]:
        c.wait()
    for c in nb:
        c.wait_recv()
    first, last = ci == 0, ci == chain_n - 1
    own = (own_in, own_mid, own_out)
    sq_a = sq_b = cross = jnp.zeros((1, 128), F32)

    def fold(v):
        v = jnp.sum(v, axis=0, keepdims=True)
        out = v[:, :128]
        for c in range(1, v.shape[1] // 128):
            out = out + v[:, c * 128 : (c + 1) * 128]
        return out

    for m, (e, b) in enumerate(((e_in, nb_in), (e_mid, nb_mid), (e_out, nb_out))):
        n = own[m].shape[1]
        o = own[m][...]
        if m == 2:
            AH[m, :, edge:] = jnp.zeros((o.shape[0], width - edge), F32)
            BH[m, :, edge:] = jnp.zeros((o.shape[0], width - edge), F32)
        AH[m, :, :n] = jnp.where(last, e[1], b[1]) - o
        BH[m, :, :n] = o - jnp.where(first, e[0], b[0])
        a, z = AH[m], BH[m]
        sq_a, sq_b, cross = sq_a + fold(a * a), sq_b + fold(z * z), cross + fold(a * z)

    def pack(*values):
        zero = jnp.zeros((4 - len(values), 128), F32)
        return jnp.concatenate([*values, zero], axis=0) if len(values) < 4 else jnp.concatenate(values, axis=0)

    me = yi * SIDE + xi
    others = [(i, j) for i in range(SIDE) for j in range(SIDE) if i or j]

    def exchange(slot, tile):
        sums[slot, me] = tile
        src = sums.at[slot, me]
        g = cp.group(sums.at[slot, pl.ds(0, len(others))])
        for i, j in others:
            g.start(src, src, {**at_y(i), **at_x(j)})
        return g

    def collect(slot, copies):
        copies.wait_recv()
        out = sums[slot, 0]
        for k in range(1, SIDE * SIDE):
            out = out + sums[slot, k]
        return jnp.sum(out, axis=1, keepdims=True)

    ag_near_end()
    ag_far(0, ACROSS)
    ag_far(1, SIDES)
    ag_far_forward(0, SIDES)
    ag_far_forward(0, ACROSS)
    ag_far(1, ACROSS)
    ag_far(2, SIDES)
    early = exchange(0, pack(sq_b, sq_a, cross))
    def forward_in(i):
        pre = mm(x[part(i), :], weight(0))
        sig = jax.nn.sigmoid(pre)
        hid[part(i), :] = (pre * sig).astype(BF16)
        slope[part(i), :] = sig * (1.0 + pre * (1.0 - sig))

    def forward_mid(i):
        r = x[part(i), :].astype(F32) + mm(hid[part(i), :], weight(1))
        resid[part(i), :] = r.astype(BF16)

    norm = 1.0 / (batch * classes)

    HALF, QUARTER = width // 2, width // 4
    PIECES = [
        (2, 0, QUARTER), (2, QUARTER, QUARTER), (2, HALF, HALF),
        (1, 0, HALF), (1, HALF, HALF), (0, 0, HALF), (0, HALF, HALF),
    ]

    def cols_of(p):
        return pl.ds(PIECES[p][1], PIECES[p][2])

    def forward_out(p, energy):
        _, first_col, n = PIECES[p]
        logits = mm(resid[...], W[2, :, :, :, :, cols_of(p)].reshape(width, n))
        for c in range(n // 128):
            at = first_col + c * 128
            hit = lcol[...] == lanes(at // 128)
            err = logits[:, c * 128 : (c + 1) * 128] - jnp.where(hit, 1.0, 0.0)
            energy = energy + jnp.sum(err * err, axis=0, keepdims=True)
            dlog[:, at : at + 128] = (err * norm).astype(BF16)
        return energy

    ag_far_forward(1, SIDES)
    ag_end(0)
    forward_in(0)
    ag_far_forward(1, ACROSS)
    ag_far(2, ACROSS)
    early = collect(0, early)
    sq_behind = jnp.broadcast_to(early[0:1], (1, 128))
    sq_ahead = jnp.broadcast_to(early[1:2], (1, 128))
    cross = jnp.broadcast_to(early[2:3], (1, 128))
    len_ahead = jnp.sqrt(sq_ahead + EPS)
    len_behind = jnp.sqrt(sq_behind + EPS)
    raw_sq = (
        sq_ahead / (len_ahead * len_ahead)
        + sq_behind / (len_behind * len_behind)
        + 2.0 * cross / (len_ahead * len_behind)
    )
    raw_len = jnp.sqrt(raw_sq + EPS)
    tau_sq = raw_sq / (raw_sq + EPS)
    chain_tab[ci] = pack(len_behind, len_ahead)
    up, down = {}, {}

    def lengths(step):
        if step > 1:
            up[step - 1].wait_recv()
        if step <= chain_n // 2:
            src = chain_tab.at[lax.rem(ci + chain_n + 1 - step, chain_n)]
            up[step] = cp.group(src)
            up[step].start(src, src, at_chain(1))
        if 1 < step <= chain_n // 2:
            down[step - 1].wait_recv()
        if step < chain_n // 2:
            src = chain_tab.at[lax.rem(ci + step - 1, chain_n)]
            down[step] = cp.group(src)
            down[step].start(src, src, at_chain(chain_n - 1))

    lengths(1)

    forward_in(1)
    ag_far_forward(2, SIDES)
    lengths(2)
    ag_end(1)
    forward_mid(0)
    ag_far_forward(2, ACROSS)
    lengths(3)
    forward_mid(1)
    lengths(4)
    ag_end(2)


    def grad(p, left, right):
        m, _, n = PIECES[p]
        g = mm_tn(left[...], right[:, cols_of(p)]).astype(BF16)
        G[m, :, :, :, :, cols_of(p)] = g.reshape(SIDE, SIDE, 2, 32, n)

    a1, a2, b1, b2 = {}, {}, {}, {}

    def rs_start(p):
        m, q = PIECES[p][0], cols_of(p)
        a1[p] = cp.group(G.at[m, pl.ds(0, 2), :, 0, :, q])
        a2[p] = cp.group(G.at[m, :, :, 0, :, q])
        for h, k in BOTH:
            dst = RA1.at[m, h, k, :, :, q]
            a1[p].start(blocks(G, m, h, 2, k, q), dst, far(h, DIRS[k]))
        for h, k in BOTH:
            dst = RAd.at[m, h, k, :, :, q]
            a2[p].start(blocks(G, m, h, DIRS[k], 1 - k, q), dst, far(h, DIRS[k]))

    def rs_far_sum(p):
        m, q = PIECES[p][0], cols_of(p)
        a1[p].wait_recv()
        for h, k in BOTH:
            mid = RA1.at[m, h, k, :, :, q]
            own_g = blocks(G, m, h, DIRS[k], k, q)
            mid[...] = (mid[...].astype(F32) + own_g[...].astype(F32)).astype(BF16)
            a2[p].start(mid, RAs.at[m, h, k, :, :, q], far(h, DIRS[k]))

    def rs_near_start(p):
        m, q = PIECES[p][0], cols_of(p)
        a2[p].wait_recv()
        b1[p] = cp.group(G.at[m, 0, pl.ds(0, 2), 0, :, q])
        b2[p] = cp.group(G.at[m, 0, :, 0, :, q])
        for h in (0, 1):
            for k in (0, 1):
                total = blocks(G, m, h, 0, k, q)[...].astype(F32)
                total = total + RAs[m, h, k, :, :, q].astype(F32)
                total = total + RAd[m, h, 1 - k, :, :, q].astype(F32)
                R1[m, h, pl.ds(2 * k, 2), :, q] = total.astype(BF16)
            step = ys if h else xs
            for k in (0, 1):
                src = R1.at[m, h, step(2), pl.ds(16 * k, 16), q]
                b1[p].start(src, RB1.at[m, h, k, :, q], near(h, DIRS[k]))
            for k in (0, 1):
                src = R1.at[m, h, step(DIRS[k]), pl.ds(16 * (1 - k), 16), q]
                b2[p].start(src, RBd.at[m, h, k, :, q], near(h, DIRS[k]))

    def rs_near_sum(p):
        m, q = PIECES[p][0], cols_of(p)
        b1[p].wait_recv()
        for h, k in BOTH:
            step = ys if h else xs
            mid = RB1.at[m, h, k, :, q]
            own_r = R1[m, h, step(DIRS[k]), pl.ds(16 * k, 16), q]
            mid[...] = (mid[...].astype(F32) + own_r.astype(F32)).astype(BF16)
            b2[p].start(mid, RBs.at[m, h, k, :, q], near(h, DIRS[k]))

    dots = [jnp.zeros((1, 128), F32)] * 3

    def rs_end(p):
        m, q = PIECES[p][0], cols_of(p)
        b2[p].wait_recv()
        for h in (0, 1):
            step = ys if h else xs
            for k in (0, 1):
                total = R1[m, h, step(0), pl.ds(16 * k, 16), q].astype(F32)
                total = total + RBs[m, h, k, :, q].astype(F32)
                total = total + RBd[m, h, 1 - k, :, q].astype(F32)
                g = total * factors[m]
                r = pl.ds(32 * h + 16 * k, 16)
                gsh[m, r, q] = g
                dots[0] = dots[0] + fold(g * AH[m, r, q])
                dots[1] = dots[1] + fold(g * BH[m, r, q])
                dots[2] = dots[2] + fold(g * g)

    def back_resid(i):
        dres[part(i), :] = mm_nt(dlog[part(i), :], weight(2)).astype(BF16)

    def back_pre(i):
        d = mm_nt(dres[part(i), :], weight(1)) * slope[part(i), :]
        dpre[part(i), :] = d.astype(BF16)

    energy = forward_out(0, jnp.zeros((1, 128), F32))
    grad(0, resid, dlog)
    rs_start(0)
    energy = forward_out(1, energy)
    grad(1, resid, dlog)
    rs_start(1)
    energy = forward_out(2, energy)
    rs_far_sum(0)
    grad(2, resid, dlog)
    rs_start(2)
    rs_far_sum(1)
    lengths(5)
    back_resid(0)
    back_resid(1)
    rs_far_sum(2)
    lengths(6)
    grad(3, hid, dres)
    rs_start(3)
    grad(4, hid, dres)
    rs_start(4)
    back_pre(0)
    rs_far_sum(3)
    lengths(7)
    back_pre(1)
    grad(5, x, dpre)
    rs_start(5)
    rs_far_sum(4)
    lengths(8)
    grad(6, x, dpre)
    rs_start(6)
    rs_near_start(0)
    rs_near_start(1)
    rs_far_sum(5)
    rs_near_start(2)
    rs_far_sum(6)
    rs_near_start(3)
    lengths(9)
    arc = jnp.zeros((1, 128), F32)
    band = jnp.zeros((1, 128), F32)
    for j in range(chain_n):
        length = chain_tab[j, 0:1]
        arc = arc + jnp.where(j <= ci, length, 0.0)
        band = band + length
    band = band + chain_tab[chain_n - 1, 1:2]
    rs_near_sum(0)
    rs_near_sum(1)
    rs_near_start(4)
    rs_near_sum(2)
    rs_near_start(5)
    rs_near_sum(3)
    rs_near_start(6)
    rs_near_sum(4)
    rs_end(0)
    rs_end(1)
    rs_end(2)
    rs_near_sum(5)
    rs_end(3)
    rs_near_sum(6)
    rs_end(4)
    rs_end(5)
    rs_end(6)

    late = collect(1, exchange(1, pack(*dots, energy)))
    g_ahead, g_behind, g_g, energy = (
        jnp.broadcast_to(late[k : k + 1], (1, 128)) for k in range(4)
    )
    along = (g_ahead / len_ahead + g_behind / len_behind) / raw_len
    count = float(chain_n)
    goal = (ci + 1).astype(F32) / (count + 1.0) * band
    climbing = jnp.full((1, 128), climb_ref[0]) == 1
    coef = jnp.where(climbing, 2.0 * along, along + SPRING * (goal - arc) / band)
    force_sq = g_g - 2.0 * coef * along + coef * coef * tau_sq
    scale = band / (count + 1.0) / jnp.sqrt(force_sq + EPS)
    wa = (scale * coef / (len_ahead * raw_len))[:, 0:1]
    wb = (scale * coef / (len_behind * raw_len))[:, 0:1]
    scale = scale[:, 0:1]
    saves = []

    def save(src, dst):
        c = pltpu.make_async_copy(src, dst, local_sem.at[10 + len(saves)])
        c.start()
        saves.append(c)

    out_tab[...] = pack(0.5 * norm * energy, arc / band, 0.5 * raw_len)
    save(out_tab, tab_ref)
    for m, (up, dst) in enumerate(((out_in, up_in), (out_mid, up_mid), (out_out, up_out))):
        n = up.shape[1]
        u = wa * AH[m, :, :n] + wb * BH[m, :, :n] - scale * gsh[m, :, :n]
        up[...] = own[m][...] + u
        save(up, dst)
    for c in cp.all:
        c.wait_send()
    for c in saves:
        c.wait()


def hand_out(up_in, up_mid, up_out, tab, new_in, new_mid, new_out, energy, share, bend):
    for up, new in ((up_in, new_in), (up_mid, new_mid), (up_out, new_out)):
        new[0] = up[...]
    energy[0], share[0], bend[0] = tab[0, 0], tab[1, 0], tab[2, 0]


def on_device(
    images_in, images_mid, images_out, ends_in, ends_mid, ends_out, data_pool, batch_rows, labels, climbing
):
    _, shard, hidden_units = images_in.shape
    width = data_pool.shape[1]
    classes = images_out.shape[2]
    rows = batch_rows.shape[1]
    pool_rows = data_pool.shape[0]
    chain_n = lax.axis_size("chain")
    batch = rows * lax.axis_size(DP)
    any_spec = pl.BlockSpec(memory_space=pl.ANY)
    vmem_spec = pl.BlockSpec(memory_space=pltpu.VMEM)
    vm = pltpu.VMEM
    scratch = [
        vm((3, SIDE, SIDE, 2, 32, width), BF16),
        vm((3, SIDE, SIDE, 2, 32, width), BF16),
        vm((3, 2, 2, 2, 32, width), BF16),
        vm((3, 2, 2, 2, 32, width), BF16),
        vm((3, 2, 2, 2, 32, width), BF16),
        vm((3, 2, SIDE, 32, width), BF16),
        vm((3, 2, 2, 16, width), BF16),
        vm((3, 2, 2, 16, width), BF16),
        vm((3, 2, 2, 16, width), BF16),
        vm((3, shard, width), F32),
        vm((shard, width), F32),
        vm((shard, width), F32),
        vm((shard, classes), F32),
        vm((2, shard, width), F32),
        vm((2, shard, width), F32),
        vm((2, shard, classes), F32),
        vm((2, shard, width), F32),
        vm((2, shard, width), F32),
        vm((2, shard, classes), F32),
        vm((3, shard, width), F32),
        vm((3, shard, width), F32),
        vm((pool_rows, width), BF16),
        vm((rows, pool_rows), BF16),
        vm((rows, 128), F32),
        vm((rows, 128), F32),
        vm((rows, width), BF16),
        vm((rows, width), BF16),
        vm((rows, width), F32),
        vm((rows, width), BF16),
        vm((rows, width), BF16),
        vm((rows, width), BF16),
        vm((rows, width), BF16),
        vm((1, rows), jnp.int32),
        vm((1, rows), jnp.int32),
        pltpu.SMEM((1,), jnp.int32),
        vm((2, SIDE * SIDE, 4, 128), F32),
        vm((chain_n, 4, 128), F32),
        vm((shard, width), F32),
        vm((shard, width), F32),
        vm((shard, classes), F32),
        vm((4, 128), F32),
        pltpu.SemaphoreType.DMA((14,)),
        pltpu.SemaphoreType.DMA((N_COPIES,)),
        pltpu.SemaphoreType.DMA((N_COPIES,)),
    ]
    up_in, up_mid, up_out, tab = pl.pallas_call(
        functools.partial(kernel, (chain_n, batch, classes)),
        out_shape=(
            jax.ShapeDtypeStruct((shard, hidden_units), F32),
            jax.ShapeDtypeStruct((shard, width), F32),
            jax.ShapeDtypeStruct((shard, classes), F32),
            jax.ShapeDtypeStruct((4, 128), F32),
        ),
        in_specs=[any_spec] * 9 + [pl.BlockSpec(memory_space=pltpu.HBM)],
        out_specs=(any_spec,) * 4,
        scratch_shapes=scratch,
        compiler_params=pltpu.CompilerParams(
            collective_id=0, has_side_effects=True, vmem_limit_bytes=56 * 2**20
        ),
        cost_estimate=pl.CostEstimate(
            flops=2 * rows * width * (8 * width + pool_rows), bytes_accessed=10**7, transcendentals=10**6
        ),
        name="band_step",
    )(images_in, images_mid, images_out, ends_in, ends_mid, ends_out, data_pool, batch_rows, labels, climbing)
    scalar = jax.ShapeDtypeStruct((1,), F32)
    smem_spec = pl.BlockSpec(memory_space=pltpu.SMEM)
    return pl.pallas_call(
        hand_out,
        out_shape=(
            jax.ShapeDtypeStruct(images_in.shape, F32),
            jax.ShapeDtypeStruct(images_mid.shape, F32),
            jax.ShapeDtypeStruct(images_out.shape, F32),
            scalar,
            scalar,
            scalar,
        ),
        in_specs=[vmem_spec] * 3 + [smem_spec],
        out_specs=(vmem_spec,) * 3 + (smem_spec,) * 3,
        name="hand_out",
    )(up_in, up_mid, up_out, tab)


def solution(mesh):
    torus = Mesh(mesh.devices.reshape(mesh.shape["chain"], SIDE, SIDE), ("chain", "dp_0", "dp_1"))
    shard = P("chain", DP, None)
    end = P(None, DP, None)
    in_specs = (
        shard, shard, shard, end, end, end, P(DP, None), P("chain", DP), P("chain", DP), P("chain"),
    )
    out_specs = (shard, shard, shard, P("chain"), P("chain"), P("chain"))
    return jax.shard_map(
        on_device, mesh=torus, in_specs=in_specs, out_specs=out_specs, check_vma=False
    )
```

```python
import functools

import jax
import jax.numpy as jnp
from jax import lax
from jax.experimental import pallas as pl
from jax.experimental.pallas import tpu as pltpu
from jax.sharding import Mesh
from jax.sharding import PartitionSpec as P

DP = ("dp_0", "dp_1")
SPRING = 0.03
EPS = 1e-06
F32 = jnp.float32
BF16 = jnp.bfloat16
SIDE = 4
N_COPIES = 64


def mm(a, b):
    return jnp.dot(a, b, preferred_element_type=F32)


def mm_nt(a, b):
    return lax.dot_general(a, b, (((1,), (1,)), ((), ())), preferred_element_type=F32)


def mm_tn(a, b):
    return lax.dot_general(a, b, (((0,), (0,)), ((), ())), preferred_element_type=F32)


class Group:
    def __init__(self, copies, whole):
        i = len(copies.all)
        self.sems = (copies.send.at[i], copies.recv.at[i])
        self.whole = whole
        copies.all.append(self)

    def _copy(self, src, dst, device):
        return pltpu.make_async_remote_copy(
            src_ref=src,
            dst_ref=dst,
            send_sem=self.sems[0],
            recv_sem=self.sems[1],
            device_id=device,
            device_id_type=pl.DeviceIdType.MESH,
        )

    def start(self, src, dst, device):
        self.device = device
        self._copy(src, dst, device).start()

    def wait_recv(self):
        self._copy(self.whole, self.whole, self.device).wait_recv()

    def wait_send(self):
        self._copy(self.whole, self.whole, self.device).wait_send()


class Copies:
    def __init__(self, send, recv):
        self.send, self.recv, self.all = send, recv, []

    def group(self, whole):
        return Group(self, whole)


def kernel(
    dims,
    im_in, im_mid, im_out, en_in, en_mid, en_out, pool_hbm, rows_hbm, labs_hbm, climb_hbm,
    up_in, up_mid, up_out, tab_ref,
    W, G, RA1, RAd, RAs, R1, RB1, RBd, RBs, gsh,
    own_in, own_mid, own_out, nb_in, nb_mid, nb_out, e_in, e_mid, e_out, AH, BH,
    pool, onehot, rcol, lcol, x, hid, slope, resid, dlog, dres, dpre,
    rows_ref, labs_ref, climb_ref, sums, chain_tab, out_in, out_mid, out_out, out_tab,
    local_sem, send_sem, recv_sem,
):
    chain_n, batch, classes = dims
    rows = x.shape[0]
    width = x.shape[1]
    half_rows = rows // 2
    ci = lax.axis_index("chain")
    yi = lax.axis_index("dp_0")
    xi = lax.axis_index("dp_1")
    cp = Copies(send_sem, recv_sem)

    def at_x(step):
        return {"dp_1": lax.rem(xi + step, SIDE)}

    def at_y(step):
        return {"dp_0": lax.rem(yi + step, SIDE)}

    def xs(step):
        return lax.rem(xi + step, SIDE)

    def ys(step):
        return lax.rem(yi + step, SIDE)

    def at_chain(step):
        return {"chain": lax.rem(ci + step, chain_n)}

    barrier = pltpu.get_barrier_semaphore()
    partners = [at_x(1), at_x(3), at_y(1), at_y(3), at_chain(1), at_chain(chain_n - 1)]
    for device in partners:
        pl.semaphore_signal(barrier, inc=1, device_id=device, device_id_type=pl.DeviceIdType.MESH)

    loads = []

    def load(src, dst):
        c = pltpu.make_async_copy(src, dst, local_sem.at[len(loads)])
        c.start()
        loads.append(c)

    load(im_in.at[0], own_in)
    load(im_mid.at[0], own_mid)
    load(im_out.at[0], own_out)
    load(pool_hbm, pool)
    load(rows_hbm, rows_ref)
    load(labs_hbm, labs_ref)
    load(climb_hbm, climb_ref)
    load(en_in, e_in)
    load(en_mid, e_mid)
    load(en_out, e_out)

    factors = (width ** (-0.5), hid.shape[1] ** (-0.5), width ** (-0.5))
    edge = classes // 128 * 128
    for m, ref in enumerate((own_in, own_mid, own_out)):
        loads[m].wait()
        if m == 2:
            W[m, yi, xi, :, :, edge:] = jnp.zeros((2, 32, width - edge), BF16)
        n = ref.shape[1]
        W[m, yi, xi, :, :, :n] = (ref[...] * factors[m]).astype(BF16).reshape(2, 32, n)
    pl.semaphore_wait(barrier, len(partners))

    DIRS = (1, 3)

    def near(h, d):
        return at_x(d) if h == 0 else at_y(d)

    def far(h, d):
        return at_y(d) if h == 0 else at_x(d)

    def piece(m, h, far_step, near_step, k=None):
        r = pl.ds(0, 32) if k is None else pl.ds(16 * k, 16)
        if h == 0:
            return W.at[m, ys(far_step), xs(near_step), h, r]
        return W.at[m, ys(near_step), xs(far_step), h, r]

    def blocks(ref, m, h, step, k, cols=None):
        two = pl.ds(2 * k, 2)
        cols = pl.ds(0, ref.shape[-1]) if cols is None else cols
        if h == 0:
            return ref.at[m, ys(step), two, 0, :, cols]
        return ref.at[m, two, xs(step), 1, :, cols]

    BOTH = [(h, k) for h in (0, 1) for k in (0, 1)]
    ALL = pl.ds(0, 3)
    near_one = cp.group(W.at[ALL, 0, :, 0])
    own_far = cp.group(W.at[ALL, 0, :, 0])
    far_one, far_fwd = {}, {}
    for h, k in BOTH:
        src = piece(ALL, h, 0, 0)
        near_one.start(src, src, near(h, DIRS[k]))
    for h, k in BOTH:
        src = piece(ALL, h, 0, 0)
        own_far.start(src, src, far(h, DIRS[k]))

    nb = []
    for own, buf in ((own_in, nb_in), (own_mid, nb_mid), (own_out, nb_out)):
        nb.append(cp.group(buf))
        nb[-1].start(own, buf.at[0], at_chain(1))
        nb[-1].start(own, buf.at[1], at_chain(chain_n - 1))

    near_fwd = cp.group(W.at[ALL, 0, pl.ds(0, 2), 0])
    own_fwd = cp.group(W.at[ALL, 0, pl.ds(0, 2), 0])

    def ag_near_forward():
        near_one.wait_recv()
        for h, k in BOTH:
            src = piece(ALL, h, 0, SIDE - DIRS[k], k)
            near_fwd.start(src, src, near(h, DIRS[k]))

    def ag_far(m, steps):
        far_one[m, steps] = cp.group(W.at[m, pl.ds(0, len(steps)), :, 0])
        for j in steps:
            for h, k in BOTH:
                src = piece(m, h, 0, j)
                far_one[m, steps].start(src, src, far(h, DIRS[k]))

    def ag_own_forward():
        own_far.wait_recv()
        for h, k in BOTH:
            src = piece(ALL, h, SIDE - DIRS[k], 0, k)
            own_fwd.start(src, src, far(h, DIRS[k]))

    def ag_near_end():
        near_fwd.wait_recv()

    def ag_far_forward(m, steps):
        far_one[m, steps].wait_recv()
        far_fwd[m, steps] = cp.group(W.at[m, 0, pl.ds(0, 2 * len(steps)), 0])
        for j in steps:
            for h, k in BOTH:
                src = piece(m, h, SIDE - DIRS[k], j, k)
                far_fwd[m, steps].start(src, src, far(h, DIRS[k]))

    def ag_end(m):
        if m == 0:
            own_fwd.wait_recv()
        far_fwd[m, SIDES].wait_recv()
        far_fwd[m, ACROSS].wait_recv()

    def weight(m):
        return W[m].reshape(width, width)

    def part(i):
        return pl.ds(i * half_rows, half_rows)

    SIDES, ACROSS = (1, 3), (2,)

    for c in loads[4:7]:
        c.wait()
    for ref, col in ((rows_ref, rcol), (labs_ref, lcol)):
        for k in range(rows // 128):
            r = pl.ds(k * 128, 128)
            col[r, :] = jnp.transpose(jnp.broadcast_to(ref[:, r].astype(F32), (128, 128)))

    def lanes(c):
        return (lax.broadcasted_iota(jnp.int32, (1, 128), 1) + 128 * c).astype(F32)

    def pick_rows(i):
        for c in range(pool.shape[0] // 128):
            hit = rcol[part(i), :] == lanes(c)
            onehot[part(i), c * 128 : (c + 1) * 128] = jnp.where(hit, 1.0, 0.0).astype(BF16)
        x[part(i), :] = mm(onehot[part(i), :], pool[...]).astype(BF16)

    loads[3].wait()
    pick_rows(0)
    ag_near_forward()
    ag_far(0, SIDES)
    pick_rows(1)
    ag_own_forward()

    for c in loads[7:]:
        c.wait()
    for c in nb:
        c.wait_recv()
    first, last = ci == 0, ci == chain_n - 1
    own = (own_in, own_mid, own_out)
    sq_a = sq_b = cross = jnp.zeros((1, 128), F32)

    def fold(v):
        v = jnp.sum(v, axis=0, keepdims=True)
        out = v[:, :128]
        for c in range(1, v.shape[1] // 128):
            out = out + v[:, c * 128 : (c + 1) * 128]
        return out

    for m, (e, b) in enumerate(((e_in, nb_in), (e_mid, nb_mid), (e_out, nb_out))):
        n = own[m].shape[1]
        o = own[m][...]
        if m == 2:
            AH[m, :, edge:] = jnp.zeros((o.shape[0], width - edge), F32)
            BH[m, :, edge:] = jnp.zeros((o.shape[0], width - edge), F32)
        AH[m, :, :n] = jnp.where(last, e[1], b[1]) - o
        BH[m, :, :n] = o - jnp.where(first, e[0], b[0])
        a, z = AH[m], BH[m]
        sq_a, sq_b, cross = sq_a + fold(a * a), sq_b + fold(z * z), cross + fold(a * z)

    def pack(*values):
        zero = jnp.zeros((4 - len(values), 128), F32)
        return jnp.concatenate([*values, zero], axis=0) if len(values) < 4 else jnp.concatenate(values, axis=0)

    me = yi * SIDE + xi
    others = [(i, j) for i in range(SIDE) for j in range(SIDE) if i or j]

    def exchange(slot, tile):
        sums[slot, me] = tile
        src = sums.at[slot, me]
        g = cp.group(sums.at[slot, pl.ds(0, len(others))])
        for i, j in others:
            g.start(src, src, {**at_y(i), **at_x(j)})
        return g

    def collect(slot, copies):
        copies.wait_recv()
        out = sums[slot, 0]
        for k in range(1, SIDE * SIDE):
            out = out + sums[slot, k]
        return jnp.sum(out, axis=1, keepdims=True)

    ag_near_end()
    ag_far(0, ACROSS)
    ag_far(1, SIDES)
    ag_far_forward(0, SIDES)
    ag_far(1, ACROSS)
    ag_far_forward(0, ACROSS)
    ag_far(2, SIDES)
    ag_far(2, ACROSS)
    def forward_in(i):
        pre = mm(x[part(i), :], weight(0))
        sig = jax.nn.sigmoid(pre)
        hid[part(i), :] = (pre * sig).astype(BF16)
        slope[part(i), :] = sig * (1.0 + pre * (1.0 - sig))

    def forward_mid(i):
        r = x[part(i), :].astype(F32) + mm(hid[part(i), :], weight(1))
        resid[part(i), :] = r.astype(BF16)

    norm = 1.0 / (batch * classes)

    HALF, QUARTER = width // 2, width // 4
    PIECES = [
        (2, 0, QUARTER), (2, QUARTER, QUARTER), (2, HALF, HALF),
        (1, 0, HALF), (1, HALF, HALF), (0, 0, HALF), (0, HALF, HALF),
    ]

    def cols_of(p):
        return pl.ds(PIECES[p][1], PIECES[p][2])

    def forward_out(p, energy):
        _, first_col, n = PIECES[p]
        logits = mm(resid[...], W[2, :, :, :, :, cols_of(p)].reshape(width, n))
        for c in range(n // 128):
            at = first_col + c * 128
            hit = lcol[...] == lanes(at // 128)
            err = logits[:, c * 128 : (c + 1) * 128] - jnp.where(hit, 1.0, 0.0)
            energy = energy + jnp.sum(err * err, axis=0, keepdims=True)
            dlog[:, at : at + 128] = (err * norm).astype(BF16)
        return energy

    ag_end(0)
    forward_in(0)
    ag_far_forward(1, SIDES)
    ag_far_forward(1, ACROSS)
    forward_in(1)
    ag_far_forward(2, SIDES)
    ag_far_forward(2, ACROSS)
    ag_end(1)
    forward_mid(0)
    forward_mid(1)
    early = exchange(0, pack(sq_b, sq_a, cross))
    ag_end(2)


    def grad(p, left, right):
        m, _, n = PIECES[p]
        g = mm_tn(left[...], right[:, cols_of(p)]).astype(BF16)
        G[m, :, :, :, :, cols_of(p)] = g.reshape(SIDE, SIDE, 2, 32, n)

    a1, a2, b1, b2 = {}, {}, {}, {}

    def rs_start(p):
        m, q = PIECES[p][0], cols_of(p)
        a1[p] = cp.group(G.at[m, pl.ds(0, 2), :, 0, :, q])
        a2[p] = cp.group(G.at[m, :, :, 0, :, q])
        for h, k in BOTH:
            dst = RA1.at[m, h, k, :, :, q]
            a1[p].start(blocks(G, m, h, 2, k, q), dst, far(h, DIRS[k]))
        for h, k in BOTH:
            dst = RAd.at[m, h, k, :, :, q]
            a2[p].start(blocks(G, m, h, DIRS[k], 1 - k, q), dst, far(h, DIRS[k]))

    def rs_far_sum(p):
        m, q = PIECES[p][0], cols_of(p)
        a1[p].wait_recv()
        for h, k in BOTH:
            mid = RA1.at[m, h, k, :, :, q]
            own_g = blocks(G, m, h, DIRS[k], k, q)
            mid[...] = (mid[...].astype(F32) + own_g[...].astype(F32)).astype(BF16)
            a2[p].start(mid, RAs.at[m, h, k, :, :, q], far(h, DIRS[k]))

    def rs_near_start(p):
        m, q = PIECES[p][0], cols_of(p)
        a2[p].wait_recv()
        b1[p] = cp.group(G.at[m, 0, pl.ds(0, 2), 0, :, q])
        b2[p] = cp.group(G.at[m, 0, :, 0, :, q])
        for h in (0, 1):
            for k in (0, 1):
                total = blocks(G, m, h, 0, k, q)[...].astype(F32)
                total = total + RAs[m, h, k, :, :, q].astype(F32)
                total = total + RAd[m, h, 1 - k, :, :, q].astype(F32)
                R1[m, h, pl.ds(2 * k, 2), :, q] = total.astype(BF16)
            step = ys if h else xs
            for k in (0, 1):
                src = R1.at[m, h, step(2), pl.ds(16 * k, 16), q]
                b1[p].start(src, RB1.at[m, h, k, :, q], near(h, DIRS[k]))
            for k in (0, 1):
                src = R1.at[m, h, step(DIRS[k]), pl.ds(16 * (1 - k), 16), q]
                b2[p].start(src, RBd.at[m, h, k, :, q], near(h, DIRS[k]))

    def rs_near_sum(p):
        m, q = PIECES[p][0], cols_of(p)
        b1[p].wait_recv()
        for h, k in BOTH:
            step = ys if h else xs
            mid = RB1.at[m, h, k, :, q]
            own_r = R1[m, h, step(DIRS[k]), pl.ds(16 * k, 16), q]
            mid[...] = (mid[...].astype(F32) + own_r.astype(F32)).astype(BF16)
            b2[p].start(mid, RBs.at[m, h, k, :, q], near(h, DIRS[k]))

    dots = [jnp.zeros((1, 128), F32)] * 3

    def rs_end(p):
        m, q = PIECES[p][0], cols_of(p)
        b2[p].wait_recv()
        for h in (0, 1):
            step = ys if h else xs
            for k in (0, 1):
                total = R1[m, h, step(0), pl.ds(16 * k, 16), q].astype(F32)
                total = total + RBs[m, h, k, :, q].astype(F32)
                total = total + RBd[m, h, 1 - k, :, q].astype(F32)
                g = total * factors[m]
                r = pl.ds(32 * h + 16 * k, 16)
                gsh[m, r, q] = g
                dots[0] = dots[0] + fold(g * AH[m, r, q])
                dots[1] = dots[1] + fold(g * BH[m, r, q])
                dots[2] = dots[2] + fold(g * g)

    def back_resid(i):
        dres[part(i), :] = mm_nt(dlog[part(i), :], weight(2)).astype(BF16)

    def back_pre(i):
        d = mm_nt(dres[part(i), :], weight(1)) * slope[part(i), :]
        dpre[part(i), :] = d.astype(BF16)

    energy = forward_out(0, jnp.zeros((1, 128), F32))
    grad(0, resid, dlog)
    rs_start(0)
    energy = forward_out(1, energy)
    grad(1, resid, dlog)
    rs_start(1)
    energy = forward_out(2, energy)
    rs_far_sum(0)
    grad(2, resid, dlog)
    rs_start(2)
    rs_far_sum(1)
    early = collect(0, early)
    sq_behind = jnp.broadcast_to(early[0:1], (1, 128))
    sq_ahead = jnp.broadcast_to(early[1:2], (1, 128))
    cross = jnp.broadcast_to(early[2:3], (1, 128))
    len_ahead = jnp.sqrt(sq_ahead + EPS)
    len_behind = jnp.sqrt(sq_behind + EPS)
    raw_sq = (
        sq_ahead / (len_ahead * len_ahead)
        + sq_behind / (len_behind * len_behind)
        + 2.0 * cross / (len_ahead * len_behind)
    )
    raw_len = jnp.sqrt(raw_sq + EPS)
    tau_sq = raw_sq / (raw_sq + EPS)
    chain_tab[ci] = pack(len_behind, len_ahead)
    up, down = {}, {}

    def lengths(step):
        if step > 1:
            up[step - 1].wait_recv()
        if step <= chain_n // 2:
            src = chain_tab.at[lax.rem(ci + chain_n + 1 - step, chain_n)]
            up[step] = cp.group(src)
            up[step].start(src, src, at_chain(1))
        if 1 < step <= chain_n // 2:
            down[step - 1].wait_recv()
        if step < chain_n // 2:
            src = chain_tab.at[lax.rem(ci + step - 1, chain_n)]
            down[step] = cp.group(src)
            down[step].start(src, src, at_chain(chain_n - 1))

    lengths(1)
    back_resid(0)
    back_resid(1)
    rs_far_sum(2)
    lengths(2)
    grad(3, hid, dres)
    rs_start(3)
    rs_near_start(0)
    lengths(3)
    grad(4, hid, dres)
    rs_start(4)
    rs_near_start(1)
    lengths(4)
    back_pre(0)
    rs_far_sum(3)
    lengths(5)
    rs_near_start(2)
    back_pre(1)
    rs_far_sum(4)
    lengths(6)
    grad(5, x, dpre)
    rs_start(5)
    rs_near_sum(0)
    rs_near_sum(1)
    lengths(7)
    grad(6, x, dpre)
    rs_start(6)
    rs_near_sum(2)
    rs_end(0)
    rs_end(1)
    lengths(8)
    rs_far_sum(5)
    rs_near_start(3)
    rs_far_sum(6)
    lengths(9)
    arc = jnp.zeros((1, 128), F32)
    band = jnp.zeros((1, 128), F32)
    for j in range(chain_n):
        length = chain_tab[j, 0:1]
        arc = arc + jnp.where(j <= ci, length, 0.0)
        band = band + length
    band = band + chain_tab[chain_n - 1, 1:2]
    rs_near_start(4)
    rs_near_start(5)
    rs_near_sum(3)
    rs_near_start(6)
    rs_near_sum(4)
    rs_end(2)
    rs_near_sum(5)
    rs_end(3)
    rs_near_sum(6)
    rs_end(4)
    rs_end(5)
    rs_end(6)

    late = collect(1, exchange(1, pack(*dots, energy)))
    g_ahead, g_behind, g_g, energy = (
        jnp.broadcast_to(late[k : k + 1], (1, 128)) for k in range(4)
    )
    along = (g_ahead / len_ahead + g_behind / len_behind) / raw_len
    count = float(chain_n)
    goal = (ci + 1).astype(F32) / (count + 1.0) * band
    climbing = jnp.full((1, 128), climb_ref[0]) == 1
    coef = jnp.where(climbing, 2.0 * along, along + SPRING * (goal - arc) / band)
    force_sq = g_g - 2.0 * coef * along + coef * coef * tau_sq
    scale = band / (count + 1.0) / jnp.sqrt(force_sq + EPS)
    wa = (scale * coef / (len_ahead * raw_len))[:, 0:1]
    wb = (scale * coef / (len_behind * raw_len))[:, 0:1]
    scale = scale[:, 0:1]
    saves = []

    def save(src, dst):
        c = pltpu.make_async_copy(src, dst, local_sem.at[10 + len(saves)])
        c.start()
        saves.append(c)

    out_tab[...] = pack(0.5 * norm * energy, arc / band, 0.5 * raw_len)
    save(out_tab, tab_ref)
    for m, (up, dst) in enumerate(((out_in, up_in), (out_mid, up_mid), (out_out, up_out))):
        n = up.shape[1]
        u = wa * AH[m, :, :n] + wb * BH[m, :, :n] - scale * gsh[m, :, :n]
        up[...] = own[m][...] + u
        save(up, dst)
    for c in cp.all:
        c.wait_send()
    for c in saves:
        c.wait()


def hand_out(up_in, up_mid, up_out, tab, new_in, new_mid, new_out, energy, share, bend):
    for up, new in ((up_in, new_in), (up_mid, new_mid), (up_out, new_out)):
        new[0] = up[...]
    energy[0], share[0], bend[0] = tab[0, 0], tab[1, 0], tab[2, 0]


def on_device(
    images_in, images_mid, images_out, ends_in, ends_mid, ends_out, data_pool, batch_rows, labels, climbing
):
    _, shard, hidden_units = images_in.shape
    width = data_pool.shape[1]
    classes = images_out.shape[2]
    rows = batch_rows.shape[1]
    pool_rows = data_pool.shape[0]
    chain_n = lax.axis_size("chain")
    batch = rows * lax.axis_size(DP)
    any_spec = pl.BlockSpec(memory_space=pl.ANY)
    vmem_spec = pl.BlockSpec(memory_space=pltpu.VMEM)
    vm = pltpu.VMEM
    scratch = [
        vm((3, SIDE, SIDE, 2, 32, width), BF16),
        vm((3, SIDE, SIDE, 2, 32, width), BF16),
        vm((3, 2, 2, 2, 32, width), BF16),
        vm((3, 2, 2, 2, 32, width), BF16),
        vm((3, 2, 2, 2, 32, width), BF16),
        vm((3, 2, SIDE, 32, width), BF16),
        vm((3, 2, 2, 16, width), BF16),
        vm((3, 2, 2, 16, width), BF16),
        vm((3, 2, 2, 16, width), BF16),
        vm((3, shard, width), F32),
        vm((shard, width), F32),
        vm((shard, width), F32),
        vm((shard, classes), F32),
        vm((2, shard, width), F32),
        vm((2, shard, width), F32),
        vm((2, shard, classes), F32),
        vm((2, shard, width), F32),
        vm((2, shard, width), F32),
        vm((2, shard, classes), F32),
        vm((3, shard, width), F32),
        vm((3, shard, width), F32),
        vm((pool_rows, width), BF16),
        vm((rows, pool_rows), BF16),
        vm((rows, 128), F32),
        vm((rows, 128), F32),
        vm((rows, width), BF16),
        vm((rows, width), BF16),
        vm((rows, width), F32),
        vm((rows, width), BF16),
        vm((rows, width), BF16),
        vm((rows, width), BF16),
        vm((rows, width), BF16),
        vm((1, rows), jnp.int32),
        vm((1, rows), jnp.int32),
        pltpu.SMEM((1,), jnp.int32),
        vm((2, SIDE * SIDE, 4, 128), F32),
        vm((chain_n, 4, 128), F32),
        vm((shard, width), F32),
        vm((shard, width), F32),
        vm((shard, classes), F32),
        vm((4, 128), F32),
        pltpu.SemaphoreType.DMA((14,)),
        pltpu.SemaphoreType.DMA((N_COPIES,)),
        pltpu.SemaphoreType.DMA((N_COPIES,)),
    ]
    up_in, up_mid, up_out, tab = pl.pallas_call(
        functools.partial(kernel, (chain_n, batch, classes)),
        out_shape=(
            jax.ShapeDtypeStruct((shard, hidden_units), F32),
            jax.ShapeDtypeStruct((shard, width), F32),
            jax.ShapeDtypeStruct((shard, classes), F32),
            jax.ShapeDtypeStruct((4, 128), F32),
        ),
        in_specs=[any_spec] * 9 + [pl.BlockSpec(memory_space=pltpu.HBM)],
        out_specs=(any_spec,) * 4,
        scratch_shapes=scratch,
        compiler_params=pltpu.CompilerParams(
            collective_id=0, has_side_effects=True, vmem_limit_bytes=56 * 2**20
        ),
        cost_estimate=pl.CostEstimate(
            flops=2 * rows * width * (8 * width + pool_rows), bytes_accessed=10**7, transcendentals=10**6
        ),
        name="band_step",
    )(images_in, images_mid, images_out, ends_in, ends_mid, ends_out, data_pool, batch_rows, labels, climbing)
    scalar = jax.ShapeDtypeStruct((1,), F32)
    smem_spec = pl.BlockSpec(memory_space=pltpu.SMEM)
    return pl.pallas_call(
        hand_out,
        out_shape=(
            jax.ShapeDtypeStruct(images_in.shape, F32),
            jax.ShapeDtypeStruct(images_mid.shape, F32),
            jax.ShapeDtypeStruct(images_out.shape, F32),
            scalar,
            scalar,
            scalar,
        ),
        in_specs=[vmem_spec] * 3 + [smem_spec],
        out_specs=(vmem_spec,) * 3 + (smem_spec,) * 3,
        name="hand_out",
    )(up_in, up_mid, up_out, tab)


def solution(mesh):
    torus = Mesh(mesh.devices.reshape(mesh.shape["chain"], SIDE, SIDE), ("chain", "dp_0", "dp_1"))
    shard = P("chain", DP, None)
    end = P(None, DP, None)
    in_specs = (
        shard, shard, shard, end, end, end, P(DP, None), P("chain", DP), P("chain", DP), P("chain"),
    )
    out_specs = (shard, shard, shard, P("chain"), P("chain"), P("chain"))
    return jax.shard_map(
        on_device, mesh=torus, in_specs=in_specs, out_specs=out_specs, check_vma=False
    )
```

```python
import functools

import jax
import jax.numpy as jnp
from jax import lax
from jax.experimental import pallas as pl
from jax.experimental.pallas import tpu as pltpu
from jax.sharding import Mesh
from jax.sharding import PartitionSpec as P

DP = ("dp_0", "dp_1")
SPRING = 0.03
EPS = 1e-06
F32 = jnp.float32
BF16 = jnp.bfloat16
SIDE = 4
N_COPIES = 64


def mm(a, b):
    return jnp.dot(a, b, preferred_element_type=F32)


def mm_nt(a, b):
    return lax.dot_general(a, b, (((1,), (1,)), ((), ())), preferred_element_type=F32)


def mm_tn(a, b):
    return lax.dot_general(a, b, (((0,), (0,)), ((), ())), preferred_element_type=F32)


class Group:
    def __init__(self, copies, whole):
        i = len(copies.all)
        self.sems = (copies.send.at[i], copies.recv.at[i])
        self.whole = whole
        copies.all.append(self)

    def _copy(self, src, dst, device):
        return pltpu.make_async_remote_copy(
            src_ref=src,
            dst_ref=dst,
            send_sem=self.sems[0],
            recv_sem=self.sems[1],
            device_id=device,
            device_id_type=pl.DeviceIdType.MESH,
        )

    def start(self, src, dst, device):
        self.device = device
        self._copy(src, dst, device).start()

    def wait_recv(self):
        self._copy(self.whole, self.whole, self.device).wait_recv()

    def wait_send(self):
        self._copy(self.whole, self.whole, self.device).wait_send()


class Copies:
    def __init__(self, send, recv):
        self.send, self.recv, self.all = send, recv, []

    def group(self, whole):
        return Group(self, whole)


def kernel(
    dims,
    im_in, im_mid, im_out, en_in, en_mid, en_out, pool_hbm, rows_hbm, labs_hbm, climb_hbm,
    up_in, up_mid, up_out, tab_ref,
    W, G, RA1, RAd, RAs, R1, RB1, RBd, RBs, gsh,
    own_in, own_mid, own_out, nb_in, nb_mid, nb_out, e_in, e_mid, e_out, AH, BH,
    pool, onehot, rcol, lcol, x, hid, slope, resid, dlog, dres, dpre,
    rows_ref, labs_ref, climb_ref, sums, chain_tab, out_tab,
    local_sem, send_sem, recv_sem,
):
    chain_n, batch, classes = dims
    rows = x.shape[0]
    width = x.shape[1]
    half_rows = rows // 2
    ci = lax.axis_index("chain")
    yi = lax.axis_index("dp_0")
    xi = lax.axis_index("dp_1")
    cp = Copies(send_sem, recv_sem)

    def at_x(step):
        return {"dp_1": lax.rem(xi + step, SIDE)}

    def at_y(step):
        return {"dp_0": lax.rem(yi + step, SIDE)}

    def xs(step):
        return lax.rem(xi + step, SIDE)

    def ys(step):
        return lax.rem(yi + step, SIDE)

    def at_chain(step):
        return {"chain": lax.rem(ci + step, chain_n)}

    barrier = pltpu.get_barrier_semaphore()
    partners = [at_x(1), at_x(3), at_y(1), at_y(3), at_chain(1), at_chain(chain_n - 1)]
    for device in partners:
        pl.semaphore_signal(barrier, inc=1, device_id=device, device_id_type=pl.DeviceIdType.MESH)

    loads = []

    def load(src, dst):
        c = pltpu.make_async_copy(src, dst, local_sem.at[len(loads)])
        c.start()
        loads.append(c)

    load(im_in.at[0], own_in)
    load(im_mid.at[0], own_mid)
    load(im_out.at[0], own_out)
    load(pool_hbm, pool)
    load(rows_hbm, rows_ref)
    load(labs_hbm, labs_ref)
    load(climb_hbm, climb_ref)
    load(en_in, e_in)
    load(en_mid, e_mid)
    load(en_out, e_out)

    factors = (width ** (-0.5), hid.shape[1] ** (-0.5), width ** (-0.5))
    edge = classes // 128 * 128
    for m, ref in enumerate((own_in, own_mid, own_out)):
        loads[m].wait()
        if m == 2:
            W[m, yi, xi, :, :, edge:] = jnp.zeros((2, 32, width - edge), BF16)
        n = ref.shape[1]
        W[m, yi, xi, :, :, :n] = (ref[...] * factors[m]).astype(BF16).reshape(2, 32, n)
    pl.semaphore_wait(barrier, len(partners))

    DIRS = (1, 3)

    def near(h, d):
        return at_x(d) if h == 0 else at_y(d)

    def far(h, d):
        return at_y(d) if h == 0 else at_x(d)

    def piece(m, h, far_step, near_step, k=None):
        r = pl.ds(0, 32) if k is None else pl.ds(16 * k, 16)
        if h == 0:
            return W.at[m, ys(far_step), xs(near_step), h, r]
        return W.at[m, ys(near_step), xs(far_step), h, r]

    def blocks(ref, m, h, step, k, cols=None):
        two = pl.ds(2 * k, 2)
        cols = pl.ds(0, ref.shape[-1]) if cols is None else cols
        if h == 0:
            return ref.at[m, ys(step), two, 0, :, cols]
        return ref.at[m, two, xs(step), 1, :, cols]

    BOTH = [(h, k) for h in (0, 1) for k in (0, 1)]
    ALL = pl.ds(0, 3)
    near_one = cp.group(W.at[ALL, 0, :, 0])
    own_far = cp.group(W.at[ALL, 0, :, 0])
    far_one, far_fwd = {}, {}
    for h, k in BOTH:
        src = piece(ALL, h, 0, 0)
        near_one.start(src, src, near(h, DIRS[k]))
    for h, k in BOTH:
        src = piece(ALL, h, 0, 0)
        own_far.start(src, src, far(h, DIRS[k]))

    nb = []
    for own, buf in ((own_in, nb_in), (own_mid, nb_mid), (own_out, nb_out)):
        nb.append(cp.group(buf))
        nb[-1].start(own, buf.at[0], at_chain(1))
        nb[-1].start(own, buf.at[1], at_chain(chain_n - 1))

    near_fwd = cp.group(W.at[ALL, 0, pl.ds(0, 2), 0])
    own_fwd = cp.group(W.at[ALL, 0, pl.ds(0, 2), 0])

    def ag_near_forward():
        near_one.wait_recv()
        for h, k in BOTH:
            src = piece(ALL, h, 0, SIDE - DIRS[k], k)
            near_fwd.start(src, src, near(h, DIRS[k]))

    def ag_far(m, steps):
        far_one[m, steps] = cp.group(W.at[m, pl.ds(0, len(steps)), :, 0])
        for j in steps:
            for h, k in BOTH:
                src = piece(m, h, 0, j)
                far_one[m, steps].start(src, src, far(h, DIRS[k]))

    def ag_own_forward():
        own_far.wait_recv()
        for h, k in BOTH:
            src = piece(ALL, h, SIDE - DIRS[k], 0, k)
            own_fwd.start(src, src, far(h, DIRS[k]))

    def ag_near_end():
        near_fwd.wait_recv()

    def ag_far_forward(m, steps):
        far_one[m, steps].wait_recv()
        far_fwd[m, steps] = cp.group(W.at[m, 0, pl.ds(0, 2 * len(steps)), 0])
        for j in steps:
            for h, k in BOTH:
                src = piece(m, h, SIDE - DIRS[k], j, k)
                far_fwd[m, steps].start(src, src, far(h, DIRS[k]))

    def ag_end(m):
        if m == 0:
            own_fwd.wait_recv()
        far_fwd[m, SIDES].wait_recv()
        far_fwd[m, ACROSS].wait_recv()

    def weight(m):
        return W[m].reshape(width, width)

    def part(i):
        return pl.ds(i * half_rows, half_rows)

    SIDES, ACROSS = (1, 3), (2,)

    for c in loads[4:7]:
        c.wait()
    for ref, col in ((rows_ref, rcol), (labs_ref, lcol)):
        for k in range(rows // 128):
            r = pl.ds(k * 128, 128)
            col[r, :] = jnp.transpose(jnp.broadcast_to(ref[:, r].astype(F32), (128, 128)))

    def lanes(c):
        return (lax.broadcasted_iota(jnp.int32, (1, 128), 1) + 128 * c).astype(F32)

    def pick_rows(i):
        for c in range(pool.shape[0] // 128):
            hit = rcol[part(i), :] == lanes(c)
            onehot[part(i), c * 128 : (c + 1) * 128] = jnp.where(hit, 1.0, 0.0).astype(BF16)
        x[part(i), :] = mm(onehot[part(i), :], pool[...]).astype(BF16)

    loads[3].wait()
    pick_rows(0)
    ag_near_forward()
    ag_far(0, SIDES)
    pick_rows(1)
    ag_own_forward()

    for c in loads[7:]:
        c.wait()
    for c in nb:
        c.wait_recv()
    first, last = ci == 0, ci == chain_n - 1
    own = (own_in, own_mid, own_out)
    sq_a = sq_b = cross = jnp.zeros((1, 128), F32)

    def fold(v):
        v = jnp.sum(v, axis=0, keepdims=True)
        out = v[:, :128]
        for c in range(1, v.shape[1] // 128):
            out = out + v[:, c * 128 : (c + 1) * 128]
        return out

    for m, (e, b) in enumerate(((e_in, nb_in), (e_mid, nb_mid), (e_out, nb_out))):
        n = own[m].shape[1]
        o = own[m][...]
        if m == 2:
            AH[m, :, edge:] = jnp.zeros((o.shape[0], width - edge), F32)
            BH[m, :, edge:] = jnp.zeros((o.shape[0], width - edge), F32)
        AH[m, :, :n] = jnp.where(last, e[1], b[1]) - o
        BH[m, :, :n] = o - jnp.where(first, e[0], b[0])
        a, z = AH[m], BH[m]
        sq_a, sq_b, cross = sq_a + fold(a * a), sq_b + fold(z * z), cross + fold(a * z)

    def pack(*values):
        zero = jnp.zeros((4 - len(values), 128), F32)
        return jnp.concatenate([*values, zero], axis=0) if len(values) < 4 else jnp.concatenate(values, axis=0)

    me = yi * SIDE + xi
    others = [(i, j) for i in range(SIDE) for j in range(SIDE) if i or j]

    def exchange(slot, tile):
        sums[slot, me] = tile
        src = sums.at[slot, me]
        g = cp.group(sums.at[slot, pl.ds(0, len(others))])
        for i, j in others:
            g.start(src, src, {**at_y(i), **at_x(j)})
        return g

    def collect(slot, copies):
        copies.wait_recv()
        out = sums[slot, 0]
        for k in range(1, SIDE * SIDE):
            out = out + sums[slot, k]
        return jnp.sum(out, axis=1, keepdims=True)

    ag_near_end()
    ag_far(0, ACROSS)
    ag_far(1, SIDES)
    ag_far_forward(0, SIDES)
    ag_far(1, ACROSS)
    ag_far_forward(0, ACROSS)
    ag_far(2, SIDES)
    ag_far(2, ACROSS)
    def forward_in(i):
        pre = mm(x[part(i), :], weight(0))
        sig = jax.nn.sigmoid(pre)
        hid[part(i), :] = (pre * sig).astype(BF16)
        slope[part(i), :] = sig * (1.0 + pre * (1.0 - sig))

    def forward_mid(i):
        r = x[part(i), :].astype(F32) + mm(hid[part(i), :], weight(1))
        resid[part(i), :] = r.astype(BF16)

    norm = 1.0 / (batch * classes)

    HALF, QUARTER = width // 2, width // 4
    PIECES = [
        (2, 0, QUARTER), (2, QUARTER, QUARTER), (2, HALF, HALF),
        (1, 0, HALF), (1, HALF, HALF), (0, 0, HALF), (0, HALF, HALF),
    ]

    def cols_of(p):
        return pl.ds(PIECES[p][1], PIECES[p][2])

    def forward_out(p, energy):
        _, first_col, n = PIECES[p]
        logits = mm(resid[...], W[2, :, :, :, :, cols_of(p)].reshape(width, n))
        for c in range(n // 128):
            at = first_col + c * 128
            hit = lcol[...] == lanes(at // 128)
            err = logits[:, c * 128 : (c + 1) * 128] - jnp.where(hit, 1.0, 0.0)
            energy = energy + jnp.sum(err * err, axis=0, keepdims=True)
            dlog[:, at : at + 128] = (err * norm).astype(BF16)
        return energy

    ag_end(0)
    forward_in(0)
    ag_far_forward(1, SIDES)
    ag_far_forward(1, ACROSS)
    forward_in(1)
    ag_far_forward(2, SIDES)
    ag_far_forward(2, ACROSS)
    ag_end(1)
    forward_mid(0)
    forward_mid(1)
    early = exchange(0, pack(sq_b, sq_a, cross))
    ag_end(2)


    def grad(p, left, right):
        m, _, n = PIECES[p]
        g = mm_tn(left[...], right[:, cols_of(p)]).astype(BF16)
        G[m, :, :, :, :, cols_of(p)] = g.reshape(SIDE, SIDE, 2, 32, n)

    a1, a2, b1, b2 = {}, {}, {}, {}

    def rs_start(p):
        m, q = PIECES[p][0], cols_of(p)
        a1[p] = cp.group(G.at[m, pl.ds(0, 2), :, 0, :, q])
        a2[p] = cp.group(G.at[m, :, :, 0, :, q])
        for h, k in BOTH:
            dst = RA1.at[m, h, k, :, :, q]
            a1[p].start(blocks(G, m, h, 2, k, q), dst, far(h, DIRS[k]))
        for h, k in BOTH:
            dst = RAd.at[m, h, k, :, :, q]
            a2[p].start(blocks(G, m, h, DIRS[k], 1 - k, q), dst, far(h, DIRS[k]))

    def rs_far_sum(p):
        m, q = PIECES[p][0], cols_of(p)
        a1[p].wait_recv()
        for h, k in BOTH:
            mid = RA1.at[m, h, k, :, :, q]
            own_g = blocks(G, m, h, DIRS[k], k, q)
            mid[...] = (mid[...].astype(F32) + own_g[...].astype(F32)).astype(BF16)
            a2[p].start(mid, RAs.at[m, h, k, :, :, q], far(h, DIRS[k]))

    def rs_near_start(p):
        m, q = PIECES[p][0], cols_of(p)
        a2[p].wait_recv()
        b1[p] = cp.group(G.at[m, 0, pl.ds(0, 2), 0, :, q])
        b2[p] = cp.group(G.at[m, 0, :, 0, :, q])
        for h in (0, 1):
            for k in (0, 1):
                total = blocks(G, m, h, 0, k, q)[...].astype(F32)
                total = total + RAs[m, h, k, :, :, q].astype(F32)
                total = total + RAd[m, h, 1 - k, :, :, q].astype(F32)
                R1[m, h, pl.ds(2 * k, 2), :, q] = total.astype(BF16)
            step = ys if h else xs
            for k in (0, 1):
                src = R1.at[m, h, step(2), pl.ds(16 * k, 16), q]
                b1[p].start(src, RB1.at[m, h, k, :, q], near(h, DIRS[k]))
            for k in (0, 1):
                src = R1.at[m, h, step(DIRS[k]), pl.ds(16 * (1 - k), 16), q]
                b2[p].start(src, RBd.at[m, h, k, :, q], near(h, DIRS[k]))

    def rs_near_sum(p):
        m, q = PIECES[p][0], cols_of(p)
        b1[p].wait_recv()
        for h, k in BOTH:
            step = ys if h else xs
            mid = RB1.at[m, h, k, :, q]
            own_r = R1[m, h, step(DIRS[k]), pl.ds(16 * k, 16), q]
            mid[...] = (mid[...].astype(F32) + own_r.astype(F32)).astype(BF16)
            b2[p].start(mid, RBs.at[m, h, k, :, q], near(h, DIRS[k]))

    dots = [jnp.zeros((1, 128), F32)] * 3

    def rs_end(p):
        m, q = PIECES[p][0], cols_of(p)
        b2[p].wait_recv()
        for h in (0, 1):
            step = ys if h else xs
            for k in (0, 1):
                total = R1[m, h, step(0), pl.ds(16 * k, 16), q].astype(F32)
                total = total + RBs[m, h, k, :, q].astype(F32)
                total = total + RBd[m, h, 1 - k, :, q].astype(F32)
                g = total * factors[m]
                r = pl.ds(32 * h + 16 * k, 16)
                gsh[m, r, q] = g
                dots[0] = dots[0] + fold(g * AH[m, r, q])
                dots[1] = dots[1] + fold(g * BH[m, r, q])
                dots[2] = dots[2] + fold(g * g)

    def back_resid(i):
        dres[part(i), :] = mm_nt(dlog[part(i), :], weight(2)).astype(BF16)

    def back_pre(i):
        d = mm_nt(dres[part(i), :], weight(1)) * slope[part(i), :]
        dpre[part(i), :] = d.astype(BF16)

    energy = forward_out(0, jnp.zeros((1, 128), F32))
    grad(0, resid, dlog)
    rs_start(0)
    energy = forward_out(1, energy)
    grad(1, resid, dlog)
    rs_start(1)
    energy = forward_out(2, energy)
    rs_far_sum(0)
    grad(2, resid, dlog)
    rs_start(2)
    rs_far_sum(1)
    early = collect(0, early)
    sq_behind = jnp.broadcast_to(early[0:1], (1, 128))
    sq_ahead = jnp.broadcast_to(early[1:2], (1, 128))
    cross = jnp.broadcast_to(early[2:3], (1, 128))
    len_ahead = jnp.sqrt(sq_ahead + EPS)
    len_behind = jnp.sqrt(sq_behind + EPS)
    raw_sq = (
        sq_ahead / (len_ahead * len_ahead)
        + sq_behind / (len_behind * len_behind)
        + 2.0 * cross / (len_ahead * len_behind)
    )
    raw_len = jnp.sqrt(raw_sq + EPS)
    tau_sq = raw_sq / (raw_sq + EPS)
    chain_tab[ci] = pack(len_behind, len_ahead)
    up, down = {}, {}

    def lengths(step):
        if step > 1:
            up[step - 1].wait_recv()
        if step <= chain_n // 2:
            src = chain_tab.at[lax.rem(ci + chain_n + 1 - step, chain_n)]
            up[step] = cp.group(src)
            up[step].start(src, src, at_chain(1))
        if 1 < step <= chain_n // 2:
            down[step - 1].wait_recv()
        if step < chain_n // 2:
            src = chain_tab.at[lax.rem(ci + step - 1, chain_n)]
            down[step] = cp.group(src)
            down[step].start(src, src, at_chain(chain_n - 1))

    lengths(1)
    back_resid(0)
    back_resid(1)
    rs_far_sum(2)
    lengths(2)
    grad(3, hid, dres)
    rs_start(3)
    rs_near_start(0)
    lengths(3)
    grad(4, hid, dres)
    rs_start(4)
    rs_near_start(1)
    lengths(4)
    back_pre(0)
    rs_far_sum(3)
    lengths(5)
    rs_near_start(2)
    back_pre(1)
    rs_far_sum(4)
    lengths(6)
    grad(5, x, dpre)
    rs_start(5)
    rs_near_sum(0)
    rs_near_sum(1)
    lengths(7)
    grad(6, x, dpre)
    rs_start(6)
    rs_near_sum(2)
    rs_end(0)
    rs_end(1)
    lengths(8)
    rs_far_sum(5)
    rs_near_start(3)
    rs_far_sum(6)
    lengths(9)
    arc = jnp.zeros((1, 128), F32)
    band = jnp.zeros((1, 128), F32)
    for j in range(chain_n):
        length = chain_tab[j, 0:1]
        arc = arc + jnp.where(j <= ci, length, 0.0)
        band = band + length
    band = band + chain_tab[chain_n - 1, 1:2]
    rs_near_start(4)
    rs_near_start(5)
    rs_near_sum(3)
    rs_near_start(6)
    rs_near_sum(4)
    rs_end(2)
    rs_near_sum(5)
    rs_end(3)
    rs_near_sum(6)
    rs_end(4)
    rs_end(5)
    rs_end(6)

    late = collect(1, exchange(1, pack(*dots, energy)))
    g_ahead, g_behind, g_g, energy = (
        jnp.broadcast_to(late[k : k + 1], (1, 128)) for k in range(4)
    )
    along = (g_ahead / len_ahead + g_behind / len_behind) / raw_len
    count = float(chain_n)
    goal = (ci + 1).astype(F32) / (count + 1.0) * band
    climbing = jnp.full((1, 128), climb_ref[0]) == 1
    coef = jnp.where(climbing, 2.0 * along, along + SPRING * (goal - arc) / band)
    force_sq = g_g - 2.0 * coef * along + coef * coef * tau_sq
    scale = band / (count + 1.0) / jnp.sqrt(force_sq + EPS)
    wa = (scale * coef / (len_ahead * raw_len))[:, 0:1]
    wb = (scale * coef / (len_behind * raw_len))[:, 0:1]
    scale = scale[:, 0:1]
    saves = []

    def save(src, dst):
        c = pltpu.make_async_copy(src, dst, local_sem.at[10 + len(saves)])
        c.start()
        saves.append(c)

    out_tab[...] = pack(0.5 * norm * energy, arc / band, 0.5 * raw_len)
    save(out_tab, tab_ref)
    for m, up in enumerate((up_in, up_mid, up_out)):
        n = up.shape[1]
        u = wa * AH[m, :, :n] + wb * BH[m, :, :n] - scale * gsh[m, :, :n]
        up[...] = own[m][...] + u
    for c in cp.all:
        c.wait_send()
    for c in saves:
        c.wait()


def hand_out(up_in, up_mid, up_out, tab, new_in, new_mid, new_out, energy, share, bend):
    for up, new in ((up_in, new_in), (up_mid, new_mid), (up_out, new_out)):
        new[0] = up[...]
    energy[0], share[0], bend[0] = tab[0, 0], tab[1, 0], tab[2, 0]


def on_device(
    images_in, images_mid, images_out, ends_in, ends_mid, ends_out, data_pool, batch_rows, labels, climbing
):
    _, shard, hidden_units = images_in.shape
    width = data_pool.shape[1]
    classes = images_out.shape[2]
    rows = batch_rows.shape[1]
    pool_rows = data_pool.shape[0]
    chain_n = lax.axis_size("chain")
    batch = rows * lax.axis_size(DP)
    any_spec = pl.BlockSpec(memory_space=pl.ANY)
    vmem_spec = pl.BlockSpec(memory_space=pltpu.VMEM)
    vm = pltpu.VMEM
    scratch = [
        vm((3, SIDE, SIDE, 2, 32, width), BF16),
        vm((3, SIDE, SIDE, 2, 32, width), BF16),
        vm((3, 2, 2, 2, 32, width), BF16),
        vm((3, 2, 2, 2, 32, width), BF16),
        vm((3, 2, 2, 2, 32, width), BF16),
        vm((3, 2, SIDE, 32, width), BF16),
        vm((3, 2, 2, 16, width), BF16),
        vm((3, 2, 2, 16, width), BF16),
        vm((3, 2, 2, 16, width), BF16),
        vm((3, shard, width), F32),
        vm((shard, width), F32),
        vm((shard, width), F32),
        vm((shard, classes), F32),
        vm((2, shard, width), F32),
        vm((2, shard, width), F32),
        vm((2, shard, classes), F32),
        vm((2, shard, width), F32),
        vm((2, shard, width), F32),
        vm((2, shard, classes), F32),
        vm((3, shard, width), F32),
        vm((3, shard, width), F32),
        vm((pool_rows, width), BF16),
        vm((rows, pool_rows), BF16),
        vm((rows, 128), F32),
        vm((rows, 128), F32),
        vm((rows, width), BF16),
        vm((rows, width), BF16),
        vm((rows, width), F32),
        vm((rows, width), BF16),
        vm((rows, width), BF16),
        vm((rows, width), BF16),
        vm((rows, width), BF16),
        vm((1, rows), jnp.int32),
        vm((1, rows), jnp.int32),
        pltpu.SMEM((1,), jnp.int32),
        vm((2, SIDE * SIDE, 4, 128), F32),
        vm((chain_n, 4, 128), F32),
        vm((4, 128), F32),
        pltpu.SemaphoreType.DMA((14,)),
        pltpu.SemaphoreType.DMA((N_COPIES,)),
        pltpu.SemaphoreType.DMA((N_COPIES,)),
    ]
    up_in, up_mid, up_out, tab = pl.pallas_call(
        functools.partial(kernel, (chain_n, batch, classes)),
        out_shape=(
            vm((shard, hidden_units), F32),
            vm((shard, width), F32),
            vm((shard, classes), F32),
            jax.ShapeDtypeStruct((4, 128), F32),
        ),
        in_specs=[any_spec] * 9 + [pl.BlockSpec(memory_space=pltpu.HBM)],
        out_specs=(vmem_spec,) * 3 + (any_spec,),
        scratch_shapes=scratch,
        compiler_params=pltpu.CompilerParams(
            collective_id=0, has_side_effects=True, vmem_limit_bytes=54 * 2**20
        ),
        cost_estimate=pl.CostEstimate(
            flops=2 * rows * width * (8 * width + pool_rows), bytes_accessed=10**7, transcendentals=10**6
        ),
        name="band_step",
    )(images_in, images_mid, images_out, ends_in, ends_mid, ends_out, data_pool, batch_rows, labels, climbing)
    scalar = jax.ShapeDtypeStruct((1,), F32)
    smem_spec = pl.BlockSpec(memory_space=pltpu.SMEM)
    return pl.pallas_call(
        hand_out,
        out_shape=(
            jax.ShapeDtypeStruct(images_in.shape, F32),
            jax.ShapeDtypeStruct(images_mid.shape, F32),
            jax.ShapeDtypeStruct(images_out.shape, F32),
            scalar,
            scalar,
            scalar,
        ),
        in_specs=[vmem_spec] * 3 + [smem_spec],
        out_specs=(vmem_spec,) * 3 + (smem_spec,) * 3,
        name="hand_out",
    )(*(pltpu.with_memory_space_constraint(up, pltpu.VMEM) for up in (up_in, up_mid, up_out)), tab)


def solution(mesh):
    torus = Mesh(mesh.devices.reshape(mesh.shape["chain"], SIDE, SIDE), ("chain", "dp_0", "dp_1"))
    shard = P("chain", DP, None)
    end = P(None, DP, None)
    in_specs = (
        shard, shard, shard, end, end, end, P(DP, None), P("chain", DP), P("chain", DP), P("chain"),
    )
    out_specs = (shard, shard, shard, P("chain"), P("chain"), P("chain"))
    return jax.shard_map(
        on_device, mesh=torus, in_specs=in_specs, out_specs=out_specs, check_vma=False
    )
```

```python
import functools

import jax
import jax.numpy as jnp
from jax import lax
from jax.experimental import pallas as pl
from jax.experimental.pallas import tpu as pltpu
from jax.sharding import Mesh
from jax.sharding import PartitionSpec as P

DP = ("dp_0", "dp_1")
SPRING = 0.03
EPS = 1e-06
F32 = jnp.float32
BF16 = jnp.bfloat16
SIDE = 4
N_COPIES = 64


def mm(a, b):
    return jnp.dot(a, b, preferred_element_type=F32)


def mm_nt(a, b):
    return lax.dot_general(a, b, (((1,), (1,)), ((), ())), preferred_element_type=F32)


def mm_tn(a, b):
    return lax.dot_general(a, b, (((0,), (0,)), ((), ())), preferred_element_type=F32)


class Group:
    def __init__(self, copies, whole):
        i = len(copies.all)
        self.sems = (copies.send.at[i], copies.recv.at[i])
        self.whole = whole
        copies.all.append(self)

    def _copy(self, src, dst, device):
        return pltpu.make_async_remote_copy(
            src_ref=src,
            dst_ref=dst,
            send_sem=self.sems[0],
            recv_sem=self.sems[1],
            device_id=device,
            device_id_type=pl.DeviceIdType.MESH,
        )

    def start(self, src, dst, device):
        self.device = device
        self._copy(src, dst, device).start()

    def wait_recv(self):
        self._copy(self.whole, self.whole, self.device).wait_recv()

    def wait_send(self):
        self._copy(self.whole, self.whole, self.device).wait_send()


class Copies:
    def __init__(self, send, recv):
        self.send, self.recv, self.all = send, recv, []

    def group(self, whole):
        return Group(self, whole)


def kernel(
    dims,
    im_in, im_mid, im_out, en_in, en_mid, en_out, pool_hbm, rows_hbm, labs_hbm, climb_hbm,
    up_in, up_mid, up_out, tab_ref,
    W, G, RA1, RAd, RAs, R1, RB1, RBd, RBs, gsh,
    own_in, own_mid, own_out, nb_in, nb_mid, nb_out, e_in, e_mid, e_out, AH, BH,
    pool, onehot, rcol, lcol, x, hid, slope, resid, dlog, dres, dpre,
    rows_ref, labs_ref, climb_ref, sums, chain_tab, out_tab,
    local_sem, send_sem, recv_sem,
):
    chain_n, batch, classes = dims
    rows = x.shape[0]
    width = x.shape[1]
    half_rows = rows // 2
    ci = lax.axis_index("chain")
    yi = lax.axis_index("dp_0")
    xi = lax.axis_index("dp_1")
    cp = Copies(send_sem, recv_sem)

    def at_x(step):
        return {"dp_1": lax.rem(xi + step, SIDE)}

    def at_y(step):
        return {"dp_0": lax.rem(yi + step, SIDE)}

    def xs(step):
        return lax.rem(xi + step, SIDE)

    def ys(step):
        return lax.rem(yi + step, SIDE)

    def at_chain(step):
        return {"chain": lax.rem(ci + step, chain_n)}

    barrier = pltpu.get_barrier_semaphore()
    partners = [at_x(1), at_x(3), at_y(1), at_y(3), at_chain(1), at_chain(chain_n - 1)]
    for device in partners:
        pl.semaphore_signal(barrier, inc=1, device_id=device, device_id_type=pl.DeviceIdType.MESH)

    loads = []

    def load(src, dst):
        c = pltpu.make_async_copy(src, dst, local_sem.at[len(loads)])
        c.start()
        loads.append(c)

    load(im_in.at[0], own_in)
    load(im_mid.at[0], own_mid)
    load(im_out.at[0], own_out)
    load(pool_hbm, pool)
    load(rows_hbm, rows_ref)
    load(labs_hbm, labs_ref)
    load(climb_hbm, climb_ref)
    load(en_in, e_in)
    load(en_mid, e_mid)
    load(en_out, e_out)

    factors = (width ** (-0.5), hid.shape[1] ** (-0.5), width ** (-0.5))
    edge = classes // 128 * 128
    for m, ref in enumerate((own_in, own_mid, own_out)):
        loads[m].wait()
        if m == 2:
            W[m, yi, xi, :, :, edge:] = jnp.zeros((2, 32, width - edge), BF16)
        n = ref.shape[1]
        W[m, yi, xi, :, :, :n] = (ref[...] * factors[m]).astype(BF16).reshape(2, 32, n)
    pl.semaphore_wait(barrier, len(partners))

    DIRS = (1, 3)

    def near(h, d):
        return at_x(d) if h == 0 else at_y(d)

    def far(h, d):
        return at_y(d) if h == 0 else at_x(d)

    def piece(m, h, far_step, near_step, k=None):
        r = pl.ds(0, 32) if k is None else pl.ds(16 * k, 16)
        if h == 0:
            return W.at[m, ys(far_step), xs(near_step), h, r]
        return W.at[m, ys(near_step), xs(far_step), h, r]

    def blocks(ref, m, h, step, k, cols=None):
        two = pl.ds(2 * k, 2)
        cols = pl.ds(0, ref.shape[-1]) if cols is None else cols
        if h == 0:
            return ref.at[m, ys(step), two, 0, :, cols]
        return ref.at[m, two, xs(step), 1, :, cols]

    BOTH = [(h, k) for h in (0, 1) for k in (0, 1)]
    ALL = pl.ds(0, 3)
    near_one = cp.group(W.at[ALL, 0, :, 0])
    own_far = cp.group(W.at[ALL, 0, :, 0])
    far_one, far_fwd = {}, {}
    for h, k in BOTH:
        src = piece(ALL, h, 0, 0)
        near_one.start(src, src, near(h, DIRS[k]))
    for h, k in BOTH:
        src = piece(ALL, h, 0, 0)
        own_far.start(src, src, far(h, DIRS[k]))

    nb = []
    for own, buf in ((own_in, nb_in), (own_mid, nb_mid), (own_out, nb_out)):
        nb.append(cp.group(buf))
        nb[-1].start(own, buf.at[0], at_chain(1))
        nb[-1].start(own, buf.at[1], at_chain(chain_n - 1))

    near_fwd = cp.group(W.at[ALL, 0, pl.ds(0, 2), 0])
    own_fwd = cp.group(W.at[ALL, 0, pl.ds(0, 2), 0])

    def ag_near_forward():
        near_one.wait_recv()
        for h, k in BOTH:
            src = piece(ALL, h, 0, SIDE - DIRS[k], k)
            near_fwd.start(src, src, near(h, DIRS[k]))

    def ag_far(m, steps):
        far_one[m, steps] = cp.group(W.at[m, pl.ds(0, len(steps)), :, 0])
        for j in steps:
            for h, k in BOTH:
                src = piece(m, h, 0, j)
                far_one[m, steps].start(src, src, far(h, DIRS[k]))

    def ag_own_forward():
        own_far.wait_recv()
        for h, k in BOTH:
            src = piece(ALL, h, SIDE - DIRS[k], 0, k)
            own_fwd.start(src, src, far(h, DIRS[k]))

    def ag_near_end():
        near_fwd.wait_recv()

    def ag_far_forward(m, steps):
        far_one[m, steps].wait_recv()
        far_fwd[m, steps] = cp.group(W.at[m, 0, pl.ds(0, 2 * len(steps)), 0])
        for j in steps:
            for h, k in BOTH:
                src = piece(m, h, SIDE - DIRS[k], j, k)
                far_fwd[m, steps].start(src, src, far(h, DIRS[k]))

    def ag_end(m):
        if m == 0:
            own_fwd.wait_recv()
        far_fwd[m, SIDES].wait_recv()
        far_fwd[m, ACROSS].wait_recv()

    def weight(m):
        return W[m].reshape(width, width)

    def part(i):
        return pl.ds(i * half_rows, half_rows)

    SIDES, ACROSS = (1, 3), (2,)

    for c in loads[4:7]:
        c.wait()
    for ref, col in ((rows_ref, rcol), (labs_ref, lcol)):
        for k in range(rows // 128):
            r = pl.ds(k * 128, 128)
            col[r, :] = jnp.transpose(jnp.broadcast_to(ref[:, r].astype(F32), (128, 128)))

    def lanes(c):
        return (lax.broadcasted_iota(jnp.int32, (1, 128), 1) + 128 * c).astype(F32)

    def pick_rows(i):
        for c in range(pool.shape[0] // 128):
            hit = rcol[part(i), :] == lanes(c)
            onehot[part(i), c * 128 : (c + 1) * 128] = jnp.where(hit, 1.0, 0.0).astype(BF16)
        x[part(i), :] = mm(onehot[part(i), :], pool[...]).astype(BF16)

    loads[3].wait()
    pick_rows(0)
    ag_near_forward()
    ag_far(0, SIDES)
    pick_rows(1)
    ag_own_forward()

    for c in loads[7:]:
        c.wait()
    for c in nb:
        c.wait_recv()
    first, last = ci == 0, ci == chain_n - 1
    own = (own_in, own_mid, own_out)
    sq_a = sq_b = cross = jnp.zeros((1, 128), F32)

    def fold(v):
        v = jnp.sum(v, axis=0, keepdims=True)
        out = v[:, :128]
        for c in range(1, v.shape[1] // 128):
            out = out + v[:, c * 128 : (c + 1) * 128]
        return out

    for m, (e, b) in enumerate(((e_in, nb_in), (e_mid, nb_mid), (e_out, nb_out))):
        n = own[m].shape[1]
        o = own[m][...]
        if m == 2:
            AH[m, :, edge:] = jnp.zeros((o.shape[0], width - edge), F32)
            BH[m, :, edge:] = jnp.zeros((o.shape[0], width - edge), F32)
        AH[m, :, :n] = jnp.where(last, e[1], b[1]) - o
        BH[m, :, :n] = o - jnp.where(first, e[0], b[0])
        a, z = AH[m], BH[m]
        sq_a, sq_b, cross = sq_a + fold(a * a), sq_b + fold(z * z), cross + fold(a * z)

    def pack(*values):
        zero = jnp.zeros((4 - len(values), 128), F32)
        return jnp.concatenate([*values, zero], axis=0) if len(values) < 4 else jnp.concatenate(values, axis=0)

    me = yi * SIDE + xi
    others = [(i, j) for i in range(SIDE) for j in range(SIDE) if i or j]

    def exchange(slot, tile):
        sums[slot, me] = tile
        src = sums.at[slot, me]
        g = cp.group(sums.at[slot, pl.ds(0, len(others))])
        for i, j in others:
            g.start(src, src, {**at_y(i), **at_x(j)})
        return g

    def collect(slot, copies):
        copies.wait_recv()
        out = sums[slot, 0]
        for k in range(1, SIDE * SIDE):
            out = out + sums[slot, k]
        return jnp.sum(out, axis=1, keepdims=True)

    ag_near_end()
    ag_far(0, ACROSS)
    ag_far(1, SIDES)
    ag_far_forward(0, SIDES)
    ag_far(1, ACROSS)
    ag_far_forward(0, ACROSS)
    ag_far(2, SIDES)
    ag_far(2, ACROSS)
    def forward_in(i):
        pre = mm(x[part(i), :], weight(0))
        sig = jax.nn.sigmoid(pre)
        hid[part(i), :] = (pre * sig).astype(BF16)
        slope[part(i), :] = sig * (1.0 + pre * (1.0 - sig))

    def forward_mid(i):
        r = x[part(i), :].astype(F32) + mm(hid[part(i), :], weight(1))
        resid[part(i), :] = r.astype(BF16)

    norm = 1.0 / (batch * classes)

    HALF, QUARTER = width // 2, width // 4
    PIECES = [
        (2, 0, QUARTER), (2, QUARTER, QUARTER), (2, HALF, HALF),
        (1, 0, HALF), (1, HALF, HALF), (0, 0, HALF), (0, HALF, HALF),
    ]

    def cols_of(p):
        return pl.ds(PIECES[p][1], PIECES[p][2])

    def forward_out(p, energy):
        _, first_col, n = PIECES[p]
        logits = mm(resid[...], W[2, :, :, :, :, cols_of(p)].reshape(width, n))
        for c in range(n // 128):
            at = first_col + c * 128
            hit = lcol[...] == lanes(at // 128)
            err = logits[:, c * 128 : (c + 1) * 128] - jnp.where(hit, 1.0, 0.0)
            energy = energy + jnp.sum(err * err, axis=0, keepdims=True)
            dlog[:, at : at + 128] = (err * norm).astype(BF16)
        return energy

    ag_far_forward(1, SIDES)
    ag_far_forward(1, ACROSS)
    ag_end(0)
    forward_in(0)
    forward_in(1)
    ag_far_forward(2, SIDES)
    ag_far_forward(2, ACROSS)
    ag_end(1)
    forward_mid(0)
    forward_mid(1)
    early = exchange(0, pack(sq_b, sq_a, cross))
    ag_end(2)


    def grad(p, left, right):
        m, _, n = PIECES[p]
        g = mm_tn(left[...], right[:, cols_of(p)]).astype(BF16)
        G[m, :, :, :, :, cols_of(p)] = g.reshape(SIDE, SIDE, 2, 32, n)

    a1, a2, b1, b2 = {}, {}, {}, {}

    def rs_start(p):
        m, q = PIECES[p][0], cols_of(p)
        a1[p] = cp.group(G.at[m, pl.ds(0, 2), :, 0, :, q])
        a2[p] = cp.group(G.at[m, :, :, 0, :, q])
        for h, k in BOTH:
            dst = RA1.at[m, h, k, :, :, q]
            a1[p].start(blocks(G, m, h, 2, k, q), dst, far(h, DIRS[k]))
        for h, k in BOTH:
            dst = RAd.at[m, h, k, :, :, q]
            a2[p].start(blocks(G, m, h, DIRS[k], 1 - k, q), dst, far(h, DIRS[k]))

    def rs_far_sum(p):
        m, q = PIECES[p][0], cols_of(p)
        a1[p].wait_recv()
        for h, k in BOTH:
            mid = RA1.at[m, h, k, :, :, q]
            own_g = blocks(G, m, h, DIRS[k], k, q)
            mid[...] = (mid[...].astype(F32) + own_g[...].astype(F32)).astype(BF16)
            a2[p].start(mid, RAs.at[m, h, k, :, :, q], far(h, DIRS[k]))

    def rs_near_start(p):
        m, q = PIECES[p][0], cols_of(p)
        a2[p].wait_recv()
        b1[p] = cp.group(G.at[m, 0, pl.ds(0, 2), 0, :, q])
        b2[p] = cp.group(G.at[m, 0, :, 0, :, q])
        for h in (0, 1):
            for k in (0, 1):
                total = blocks(G, m, h, 0, k, q)[...].astype(F32)
                total = total + RAs[m, h, k, :, :, q].astype(F32)
                total = total + RAd[m, h, 1 - k, :, :, q].astype(F32)
                R1[m, h, pl.ds(2 * k, 2), :, q] = total.astype(BF16)
            step = ys if h else xs
            for k in (0, 1):
                src = R1.at[m, h, step(2), pl.ds(16 * k, 16), q]
                b1[p].start(src, RB1.at[m, h, k, :, q], near(h, DIRS[k]))
            for k in (0, 1):
                src = R1.at[m, h, step(DIRS[k]), pl.ds(16 * (1 - k), 16), q]
                b2[p].start(src, RBd.at[m, h, k, :, q], near(h, DIRS[k]))

    def rs_near_sum(p):
        m, q = PIECES[p][0], cols_of(p)
        b1[p].wait_recv()
        for h, k in BOTH:
            step = ys if h else xs
            mid = RB1.at[m, h, k, :, q]
            own_r = R1[m, h, step(DIRS[k]), pl.ds(16 * k, 16), q]
            mid[...] = (mid[...].astype(F32) + own_r.astype(F32)).astype(BF16)
            b2[p].start(mid, RBs.at[m, h, k, :, q], near(h, DIRS[k]))

    dots = [jnp.zeros((1, 128), F32)] * 3

    def rs_end(p):
        m, q = PIECES[p][0], cols_of(p)
        b2[p].wait_recv()
        for h in (0, 1):
            step = ys if h else xs
            for k in (0, 1):
                total = R1[m, h, step(0), pl.ds(16 * k, 16), q].astype(F32)
                total = total + RBs[m, h, k, :, q].astype(F32)
                total = total + RBd[m, h, 1 - k, :, q].astype(F32)
                g = total * factors[m]
                r = pl.ds(32 * h + 16 * k, 16)
                gsh[m, r, q] = g
                dots[0] = dots[0] + fold(g * AH[m, r, q])
                dots[1] = dots[1] + fold(g * BH[m, r, q])
                dots[2] = dots[2] + fold(g * g)

    def back_resid(i):
        dres[part(i), :] = mm_nt(dlog[part(i), :], weight(2)).astype(BF16)

    def back_pre(i):
        d = mm_nt(dres[part(i), :], weight(1)) * slope[part(i), :]
        dpre[part(i), :] = d.astype(BF16)

    energy = forward_out(0, jnp.zeros((1, 128), F32))
    grad(0, resid, dlog)
    rs_start(0)
    energy = forward_out(1, energy)
    grad(1, resid, dlog)
    rs_start(1)
    energy = forward_out(2, energy)
    rs_far_sum(0)
    grad(2, resid, dlog)
    rs_start(2)
    rs_far_sum(1)
    early = collect(0, early)
    sq_behind = jnp.broadcast_to(early[0:1], (1, 128))
    sq_ahead = jnp.broadcast_to(early[1:2], (1, 128))
    cross = jnp.broadcast_to(early[2:3], (1, 128))
    len_ahead = jnp.sqrt(sq_ahead + EPS)
    len_behind = jnp.sqrt(sq_behind + EPS)
    raw_sq = (
        sq_ahead / (len_ahead * len_ahead)
        + sq_behind / (len_behind * len_behind)
        + 2.0 * cross / (len_ahead * len_behind)
    )
    raw_len = jnp.sqrt(raw_sq + EPS)
    tau_sq = raw_sq / (raw_sq + EPS)
    chain_tab[ci] = pack(len_behind, len_ahead)
    up, down = {}, {}

    def lengths(step):
        if step > 1:
            up[step - 1].wait_recv()
        if step <= chain_n // 2:
            src = chain_tab.at[lax.rem(ci + chain_n + 1 - step, chain_n)]
            up[step] = cp.group(src)
            up[step].start(src, src, at_chain(1))
        if 1 < step <= chain_n // 2:
            down[step - 1].wait_recv()
        if step < chain_n // 2:
            src = chain_tab.at[lax.rem(ci + step - 1, chain_n)]
            down[step] = cp.group(src)
            down[step].start(src, src, at_chain(chain_n - 1))

    lengths(1)
    back_resid(0)
    back_resid(1)
    rs_far_sum(2)
    lengths(2)
    grad(3, hid, dres)
    rs_start(3)
    rs_near_start(0)
    lengths(3)
    grad(4, hid, dres)
    rs_start(4)
    rs_near_start(1)
    lengths(4)
    back_pre(0)
    rs_far_sum(3)
    lengths(5)
    rs_near_start(2)
    back_pre(1)
    rs_far_sum(4)
    lengths(6)
    grad(5, x, dpre)
    rs_start(5)
    rs_near_sum(0)
    rs_near_sum(1)
    lengths(7)
    grad(6, x, dpre)
    rs_start(6)
    rs_near_sum(2)
    rs_end(0)
    rs_end(1)
    lengths(8)
    rs_far_sum(5)
    rs_near_start(3)
    rs_far_sum(6)
    lengths(9)
    arc = jnp.zeros((1, 128), F32)
    band = jnp.zeros((1, 128), F32)
    for j in range(chain_n):
        length = chain_tab[j, 0:1]
        arc = arc + jnp.where(j <= ci, length, 0.0)
        band = band + length
    band = band + chain_tab[chain_n - 1, 1:2]
    rs_near_start(4)
    rs_near_start(5)
    rs_near_sum(3)
    rs_near_start(6)
    rs_near_sum(4)
    rs_end(2)
    rs_near_sum(5)
    rs_end(3)
    rs_near_sum(6)
    rs_end(4)
    rs_end(5)
    rs_end(6)

    late = collect(1, exchange(1, pack(*dots, energy)))
    g_ahead, g_behind, g_g, energy = (
        jnp.broadcast_to(late[k : k + 1], (1, 128)) for k in range(4)
    )
    along = (g_ahead / len_ahead + g_behind / len_behind) / raw_len
    count = float(chain_n)
    goal = (ci + 1).astype(F32) / (count + 1.0) * band
    climbing = jnp.full((1, 128), climb_ref[0]) == 1
    coef = jnp.where(climbing, 2.0 * along, along + SPRING * (goal - arc) / band)
    force_sq = g_g - 2.0 * coef * along + coef * coef * tau_sq
    scale = band / (count + 1.0) / jnp.sqrt(force_sq + EPS)
    wa = (scale * coef / (len_ahead * raw_len))[:, 0:1]
    wb = (scale * coef / (len_behind * raw_len))[:, 0:1]
    scale = scale[:, 0:1]
    saves = []

    def save(src, dst):
        c = pltpu.make_async_copy(src, dst, local_sem.at[10 + len(saves)])
        c.start()
        saves.append(c)

    out_tab[...] = pack(0.5 * norm * energy, arc / band, 0.5 * raw_len)
    save(out_tab, tab_ref)
    for m, up in enumerate((up_in, up_mid, up_out)):
        n = up.shape[1]
        u = wa * AH[m, :, :n] + wb * BH[m, :, :n] - scale * gsh[m, :, :n]
        up[...] = own[m][...] + u
    for c in cp.all:
        c.wait_send()
    for c in saves:
        c.wait()


def hand_out(up_in, up_mid, up_out, tab, new_in, new_mid, new_out, energy, share, bend):
    for up, new in ((up_in, new_in), (up_mid, new_mid), (up_out, new_out)):
        new[0] = up[...]
    energy[0], share[0], bend[0] = tab[0, 0], tab[1, 0], tab[2, 0]


def on_device(
    images_in, images_mid, images_out, ends_in, ends_mid, ends_out, data_pool, batch_rows, labels, climbing
):
    _, shard, hidden_units = images_in.shape
    width = data_pool.shape[1]
    classes = images_out.shape[2]
    rows = batch_rows.shape[1]
    pool_rows = data_pool.shape[0]
    chain_n = lax.axis_size("chain")
    batch = rows * lax.axis_size(DP)
    any_spec = pl.BlockSpec(memory_space=pl.ANY)
    vmem_spec = pl.BlockSpec(memory_space=pltpu.VMEM)
    vm = pltpu.VMEM
    scratch = [
        vm((3, SIDE, SIDE, 2, 32, width), BF16),
        vm((3, SIDE, SIDE, 2, 32, width), BF16),
        vm((3, 2, 2, 2, 32, width), BF16),
        vm((3, 2, 2, 2, 32, width), BF16),
        vm((3, 2, 2, 2, 32, width), BF16),
        vm((3, 2, SIDE, 32, width), BF16),
        vm((3, 2, 2, 16, width), BF16),
        vm((3, 2, 2, 16, width), BF16),
        vm((3, 2, 2, 16, width), BF16),
        vm((3, shard, width), F32),
        vm((shard, width), F32),
        vm((shard, width), F32),
        vm((shard, classes), F32),
        vm((2, shard, width), F32),
        vm((2, shard, width), F32),
        vm((2, shard, classes), F32),
        vm((2, shard, width), F32),
        vm((2, shard, width), F32),
        vm((2, shard, classes), F32),
        vm((3, shard, width), F32),
        vm((3, shard, width), F32),
        vm((pool_rows, width), BF16),
        vm((rows, pool_rows), BF16),
        vm((rows, 128), F32),
        vm((rows, 128), F32),
        vm((rows, width), BF16),
        vm((rows, width), BF16),
        vm((rows, width), F32),
        vm((rows, width), BF16),
        vm((rows, width), BF16),
        vm((rows, width), BF16),
        vm((rows, width), BF16),
        vm((1, rows), jnp.int32),
        vm((1, rows), jnp.int32),
        pltpu.SMEM((1,), jnp.int32),
        vm((2, SIDE * SIDE, 4, 128), F32),
        vm((chain_n, 4, 128), F32),
        vm((4, 128), F32),
        pltpu.SemaphoreType.DMA((14,)),
        pltpu.SemaphoreType.DMA((N_COPIES,)),
        pltpu.SemaphoreType.DMA((N_COPIES,)),
    ]
    up_in, up_mid, up_out, tab = pl.pallas_call(
        functools.partial(kernel, (chain_n, batch, classes)),
        out_shape=(
            vm((shard, hidden_units), F32),
            vm((shard, width), F32),
            vm((shard, classes), F32),
            jax.ShapeDtypeStruct((4, 128), F32),
        ),
        in_specs=[any_spec] * 9 + [pl.BlockSpec(memory_space=pltpu.HBM)],
        out_specs=(vmem_spec,) * 3 + (any_spec,),
        scratch_shapes=scratch,
        compiler_params=pltpu.CompilerParams(
            collective_id=0, has_side_effects=True, vmem_limit_bytes=54 * 2**20
        ),
        cost_estimate=pl.CostEstimate(
            flops=2 * rows * width * (8 * width + pool_rows), bytes_accessed=10**7, transcendentals=10**6
        ),
        name="band_step",
    )(images_in, images_mid, images_out, ends_in, ends_mid, ends_out, data_pool, batch_rows, labels, climbing)
    scalar = jax.ShapeDtypeStruct((1,), F32)
    smem_spec = pl.BlockSpec(memory_space=pltpu.SMEM)
    return pl.pallas_call(
        hand_out,
        out_shape=(
            jax.ShapeDtypeStruct(images_in.shape, F32),
            jax.ShapeDtypeStruct(images_mid.shape, F32),
            jax.ShapeDtypeStruct(images_out.shape, F32),
            scalar,
            scalar,
            scalar,
        ),
        in_specs=[vmem_spec] * 3 + [smem_spec],
        out_specs=(vmem_spec,) * 3 + (smem_spec,) * 3,
        name="hand_out",
    )(*(pltpu.with_memory_space_constraint(up, pltpu.VMEM) for up in (up_in, up_mid, up_out)), tab)


def solution(mesh):
    torus = Mesh(mesh.devices.reshape(mesh.shape["chain"], SIDE, SIDE), ("chain", "dp_0", "dp_1"))
    shard = P("chain", DP, None)
    end = P(None, DP, None)
    in_specs = (
        shard, shard, shard, end, end, end, P(DP, None), P("chain", DP), P("chain", DP), P("chain"),
    )
    out_specs = (shard, shard, shard, P("chain"), P("chain"), P("chain"))
    return jax.shard_map(
        on_device, mesh=torus, in_specs=in_specs, out_specs=out_specs, check_vma=False
    )
```
